32 devices in a mesh: rows: 8 (over y, x, core), rep: 4 (over z).
Axes of the slice: x: 2, y: 2, z: 4, core: 2. Of those that a mesh axis runs over, the one named last changes fastest.
Arguments:
- maps: float32 [4, 4096, 4096], P('rep', 'rows'), may hold values from -12 to 12
- mask: int32 [4096, 4096], P('rows'), may hold values 0 or 1
- bins: int32 [4096, 4096], P(None, 'rows'), may hold values from 0 to 1023
Outputs:
- spectra: float32 [2, 3, 1024], replicated
The draws below stay inside these ranges and needn't reach their ends.
All inputs are finite; a program needn't handle non-finite values. No bound on the sum of `mask` on one device may be relied on, other than what follows from the above.
Results may differ from the reference program's by a relative error of at most 0.0016.
Values sent between devices are 32-bit elements; how exact they have to be, the bound alone decides.
No kernel may reach another device: no remote copies, remote signals or barrier semaphores. Data moves between devices by JAX's collectives and lax.ppermute only.
A program may use at most 128 MiB of HBM per device.

```python
import math
import jax
import jax.numpy as jnp
from jax import lax

SIDE = 4096
NBINS = 1024
SIMS = 2


def draw_bins(key, part):
    indices = lax.iota(jnp.int32, SIDE)
    signed = jnp.where(indices >= SIDE // 2, indices - SIDE, indices)
    squared = signed[:, None] * signed[:, None] + signed[None, :] * signed[None, :]
    radial = jnp.zeros_like(squared)
    for shift_bits in range(14, -1, -1):
        candidate = radial + (1 << shift_bits)
        radial = jnp.where(candidate * candidate <= squared, candidate, radial)
    offsets = jax.random.randint(jax.random.fold_in(key, 11), (SIDE, SIDE), -1, 2, dtype=jnp.int32)
    radius_cap = SIDE * 181 // 256 + 1
    return jnp.clip((radial + offsets) * NBINS // radius_cap, 0, NBINS - 1).astype(jnp.int32)


def sky_pair(key):
    mode_count = 16
    reach = max(24 * SIDE // NBINS, 4)
    keys = jax.random.split(key, 5)
    total = 2 * mode_count
    wave_y = jax.random.randint(keys[0], (total,), -reach, reach + 1, dtype=jnp.int32)
    wave_x = jax.random.randint(keys[1], (total,), -reach, reach + 1, dtype=jnp.int32)
    wave_x = jnp.where((wave_x == 0) & (wave_y == 0), 1, wave_x)
    strength = 1.5 / math.sqrt(NBINS) * jnp.exp(jax.random.uniform(keys[2], (total,), jnp.float32, -0.7, 0.7))
    phases = jax.random.uniform(keys[3], (total,), jnp.float32, -math.pi, math.pi)
    leakage = jax.random.uniform(keys[4], (total,), jnp.float32, -1.0, 1.0) * (math.sqrt(NBINS) / SIDE)
    float_y = wave_y.astype(jnp.float32)
    float_x = wave_x.astype(jnp.float32)
    squared = float_x * float_x + float_y * float_y
    cos_twice = (float_x * float_x - float_y * float_y) / squared
    sin_twice = 2.0 * float_x * float_y / squared
    is_curl = lax.iota(jnp.int32, total) >= mode_count
    q_amp = jnp.where(is_curl, -sin_twice, cos_twice - leakage * sin_twice) * strength
    u_amp = jnp.where(is_curl, cos_twice, sin_twice + leakage * cos_twice) * strength
    cells = lax.iota(jnp.int32, SIDE)
    along_y = jnp.mod(cells[:, None] * wave_y[None, :], SIDE).astype(jnp.float32) * (2.0 * math.pi / SIDE) + phases[None, :]
    along_x = jnp.mod(wave_x[:, None] * cells[None, :], SIDE).astype(jnp.float32) * (2.0 * math.pi / SIDE)
    right_factor = jnp.concatenate([jnp.cos(along_x), -jnp.sin(along_x)], axis=0)
    left_q = jnp.concatenate([jnp.cos(along_y) * q_amp[None, :], jnp.sin(along_y) * q_amp[None, :]], axis=1)
    left_u = jnp.concatenate([jnp.cos(along_y) * u_amp[None, :], jnp.sin(along_y) * u_amp[None, :]], axis=1)
    field_q = jnp.dot(left_q, right_factor, precision=lax.Precision.HIGHEST)
    field_u = jnp.dot(left_u, right_factor, precision=lax.Precision.HIGHEST)
    return (field_q, field_u)


def draw_maps(key, part):
    noise_key = jax.random.fold_in(key, 3)
    noise = jnp.clip(jax.random.normal(noise_key, (2 * SIMS, SIDE, SIDE), jnp.float32), -5.0, 5.0)
    fields = []
    for sky in range(SIMS):
        field_q, field_u = sky_pair(jax.random.fold_in(key, 100 + sky))
        fields.append(field_q)
        fields.append(field_u)
    return jnp.clip(noise + jnp.stack(fields), -12.0, 12.0)


def with_ends(values, rng, smallest, top_value):
    index_at = [jax.random.randint(jax.random.fold_in(rng, axis), (), 0, length) for axis, length in enumerate(values.shape)]
    longest = values.shape.index(max(values.shape))
    beside = index_at[:longest] + [(index_at[longest] + 1) % values.shape[longest]] + index_at[longest + 1:]
    return values.at[tuple(index_at)].set(smallest).at[tuple(beside)].set(top_value)


def setup_inputs(seed: int = 0) -> dict:
    splits = jax.random.split(jax.random.key(seed), 4)
    maps = draw_maps(jax.random.fold_in(splits[3], 71), 0)
    mask = with_ends((jax.random.randint(splits[1], (SIDE, SIDE), 0, 4) < 3).astype(jnp.int32), jax.random.fold_in(splits[1], 1), 0, 1)
    bins = draw_bins(jax.random.fold_in(splits[3], 71), 0)
    return dict(maps=maps, mask=mask, bins=bins)


def reference(maps, mask, bins):
    extent = maps.shape[1]
    weight = mask.astype(jnp.float32)
    indices = jnp.arange(extent, dtype=jnp.int32)
    signed = jnp.where(indices >= extent // 2, indices - extent, indices).astype(jnp.float32)
    freq_y = signed[:, None]
    freq_x = signed[None, :]
    radius = jnp.maximum(freq_x * freq_x + freq_y * freq_y, 1.0)
    cos_twice = (freq_x * freq_x - freq_y * freq_y) / radius
    sin_twice = 2.0 * freq_x * freq_y / radius
    inv_area = 1.0 / (extent * extent)
    flat_bins = bins.reshape(-1)

    def one_sky(couple):
        spec_q = jnp.fft.fft2(couple[0] * weight)
        spec_u = jnp.fft.fft2(couple[1] * weight)
        q_real = jnp.real(spec_q).astype(jnp.float32)
        q_imag = jnp.imag(spec_q).astype(jnp.float32)
        u_real = jnp.real(spec_u).astype(jnp.float32)
        u_imag = jnp.imag(spec_u).astype(jnp.float32)
        e_real = cos_twice * q_real + sin_twice * u_real
        e_imag = cos_twice * q_imag + sin_twice * u_imag
        b_real = -sin_twice * q_real + cos_twice * u_real
        b_imag = -sin_twice * q_imag + cos_twice * u_imag
        powers = jnp.stack([(e_real * e_real + e_imag * e_imag) * inv_area, (b_real * b_real + b_imag * b_imag) * inv_area, (e_real * b_real + e_imag * b_imag) * inv_area])
        rounded = lax.optimization_barrier(powers.astype(jnp.bfloat16)).astype(jnp.float32)
        return jax.vmap(lambda values: jax.ops.segment_sum(values.reshape(-1), flat_bins, num_segments=NBINS))(rounded)
    sums = lax.map(one_sky, maps.reshape(SIMS, 2, extent, extent))
    auto = NBINS / (extent * extent)
    cross = math.sqrt(auto)
    factors = jnp.array([auto, auto, cross], jnp.float32)[None, :, None]
    return sums * factors
```

```python
import functools
import math

import jax
import jax.numpy as jnp
import numpy as np
from jax import lax
from jax.experimental import pallas as pl
from jax.experimental.pallas import tpu as pltpu
from jax.sharding import PartitionSpec as P

NBINS = 1024


precise = lax.Precision.HIGHEST


def partner(array, axis, distance):
    return lax.ppermute(array, axis, [(i, i ^ 1 << distance) for i in range(lax.axis_size(axis))])


def dft_table(count_a, count_b, period):
    first = lax.iota(jnp.int32, count_a)[:, None]
    second = lax.iota(jnp.int32, count_b)[None, :]
    angles = (first * second % period).astype(jnp.float32) * (2.0 * math.pi / period)
    return (jnp.cos(angles), -jnp.sin(angles))


def split_length(length):
    outer_len = 2 ** ((length.bit_length() - 1) // 2)
    return (outer_len, length // outer_len)


def complex_apply(form, real_part, imag_part, table_cos, table_sin):

    def product(left, right):
        return jnp.einsum(form, left, right, precision=precise)

    return (
        product(real_part, table_cos) - product(imag_part, table_sin),
        product(real_part, table_sin) + product(imag_part, table_cos),
    )


def twiddled(real_part, imag_part, table_cos, table_sin):
    return (
        real_part * table_cos - imag_part * table_sin,
        real_part * table_sin + imag_part * table_cos,
    )


def row_transform(values):
    count, length = values.shape
    outer_len, inner_len = split_length(length)
    outer_cos, outer_sin = dft_table(outer_len, outer_len, outer_len)
    inner_cos, inner_sin = dft_table(inner_len, inner_len, inner_len)
    turn_cos, turn_sin = dft_table(outer_len, inner_len, length)
    shaped = values.reshape(count, outer_len, inner_len)
    first_real = jnp.einsum("yan,ak->ykn", shaped, outer_cos, precision=precise)
    first_imag = jnp.einsum("yan,ak->ykn", shaped, outer_sin, precision=precise)
    mid_real, mid_imag = twiddled(first_real, first_imag, turn_cos, turn_sin)
    last_real, last_imag = complex_apply("ykn,nm->ymk", mid_real, mid_imag, inner_cos, inner_sin)
    return (last_real.reshape(count, length), last_imag.reshape(count, length))


def column_transform(pieces):
    real_part, imag_part = pieces
    length, groups, width = real_part.shape
    outer_len, inner_len = split_length(length)
    outer_cos, outer_sin = dft_table(outer_len, outer_len, outer_len)
    inner_cos, inner_sin = dft_table(inner_len, inner_len, inner_len)
    turn_cos, turn_sin = dft_table(outer_len, inner_len, length)
    shaped_real = real_part.reshape(outer_len, inner_len, groups, width)
    shaped_imag = imag_part.reshape(outer_len, inner_len, groups, width)
    first_real, first_imag = complex_apply(
        "anbc,ak->knbc", shaped_real, shaped_imag, outer_cos, outer_sin
    )
    mid_real, mid_imag = twiddled(
        first_real, first_imag, turn_cos[:, :, None, None], turn_sin[:, :, None, None]
    )
    last_real, last_imag = complex_apply("knbc,nm->mkbc", mid_real, mid_imag, inner_cos, inner_sin)
    return (last_real.reshape(length, groups, width), last_imag.reshape(length, groups, width))


def signed_float(indices, extent):
    return jnp.where(indices >= extent // 2, indices - extent, indices).astype(jnp.float32)


def band_terms(fields, freq_y, freq_x, bin_block, nbins_count, extent):
    q_real, q_imag, u_real, u_imag = fields
    radius = jnp.maximum(freq_x * freq_x + freq_y * freq_y, 1.0)
    cos_twice = (freq_x * freq_x - freq_y * freq_y) / radius
    sin_twice = 2.0 * freq_x * freq_y / radius
    e_real = cos_twice * q_real + sin_twice * u_real
    e_imag = cos_twice * q_imag + sin_twice * u_imag
    b_real = -sin_twice * q_real + cos_twice * u_real
    b_imag = -sin_twice * q_imag + cos_twice * u_imag
    inv_area = 1.0 / (extent * extent)
    powers = jnp.stack(
        [
            (e_real * e_real + e_imag * e_imag) * inv_area,
            (b_real * b_real + b_imag * b_imag) * inv_area,
            (e_real * b_real + e_imag * b_imag) * inv_area,
        ]
    ).astype(jnp.bfloat16)
    bit_count = nbins_count.bit_length() - 1
    high_count = 2 ** max(bit_count // 2 - 1, 0)
    low_count = nbins_count // high_count
    high_part = bin_block // low_count
    low_part = bin_block % low_count
    high_hot = (high_part[None] == lax.iota(jnp.int32, high_count)[:, None, None]).astype(
        jnp.bfloat16
    )
    weighted = (powers[:, None] * high_hot[None]).reshape(3 * high_count, -1)
    low_hot = (low_part[None] == lax.iota(jnp.int32, low_count)[:, None, None]).astype(jnp.bfloat16)
    low_hot = low_hot.reshape(low_count, -1)
    sums = lax.dot_general(
        weighted, low_hot, (((1,), (1,)), ((), ())), preferred_element_type=jnp.float32
    )
    return sums.reshape(3, nbins_count)


def on_device(maps, mask, bins):
    extent = bins.shape[0]
    columns = bins.shape[1]
    count = maps.shape[1]
    slab_index = lax.axis_index("rows")
    member = lax.axis_index("rep")
    pair_bit = member % 2
    field = maps[0] * mask.astype(jnp.float32)
    row_real, row_imag = row_transform(field)
    half_rows = extent // 2
    slabs = (
        row_real.reshape(count, extent // columns, columns),
        row_imag.reshape(count, extent // columns, columns),
    )
    spec_real, spec_imag = column_transform(
        (
            lax.all_to_all(slabs[0], "rows", split_axis=1, concat_axis=0, tiled=True),
            lax.all_to_all(slabs[1], "rows", split_axis=1, concat_axis=0, tiled=True),
        )
    )
    spec_real = spec_real.reshape(extent, columns)
    spec_imag = spec_imag.reshape(extent, columns)
    kept_real = lax.dynamic_slice_in_dim(spec_real, pair_bit * half_rows, half_rows, 0)
    kept_imag = lax.dynamic_slice_in_dim(spec_imag, pair_bit * half_rows, half_rows, 0)
    sent_real = lax.dynamic_slice_in_dim(spec_real, (1 - pair_bit) * half_rows, half_rows, 0)
    sent_imag = lax.dynamic_slice_in_dim(spec_imag, (1 - pair_bit) * half_rows, half_rows, 0)
    got_real, got_imag = partner((sent_real, sent_imag), "rep", 0)
    is_first = pair_bit == 0
    fields = (
        jnp.where(is_first, kept_real, got_real),
        jnp.where(is_first, kept_imag, got_imag),
        jnp.where(is_first, got_real, kept_real),
        jnp.where(is_first, got_imag, kept_imag),
    )
    own_bins = lax.dynamic_slice_in_dim(bins, pair_bit * half_rows, half_rows, 0)

    def frequency_of(offset, height):
        rows_here = lax.iota(jnp.int32, height)[:, None] + offset + pair_bit * half_rows
        cols_here = lax.iota(jnp.int32, columns)[None, :] + slab_index * columns
        return (rows_here, cols_here)

    block = min(256, half_rows)
    blocks = half_rows // block
    stacked = tuple((part.reshape(blocks, block, columns) for part in fields))
    bin_blocks = own_bins.reshape(blocks, block, columns)

    def accumulate(running, items):
        block_index, parts, bin_block = items
        rows_here, cols_here = frequency_of(block_index * block, block)
        term = band_terms(
            parts,
            signed_float(rows_here, extent),
            signed_float(cols_here, extent),
            bin_block,
            NBINS,
            extent,
        )
        return (running + term, None)

    partial_sums, _ = lax.scan(
        accumulate,
        jnp.zeros((3, NBINS), jnp.float32),
        (lax.iota(jnp.int32, blocks), stacked, bin_blocks),
    )
    sims_count = lax.axis_size("rep") // 2
    slot = (lax.iota(jnp.int32, sims_count) == member // 2).astype(jnp.float32)[:, None, None]
    totals = lax.psum(slot * partial_sums[None], ("rows", "rep"))
    auto = NBINS / (extent * extent)
    cross = math.sqrt(auto)
    factors = jnp.array([auto, auto, cross], jnp.float32)[None, :, None]
    return totals * factors


LANES = 128
OUTER = 32
HALF = LANES // 2
GROUPS = 16
LOWS = 64


def fft_wave(index, size):
    return (math.cos(2 * math.pi * index / size), -math.sin(2 * math.pi * index / size))


def turned(value, index, size):
    real, imag = value
    if index == 0:
        return value
    if 4 * index == size:
        return (imag, -real)
    cosine, sine = fft_wave(index, size)
    if 8 * index == size:
        return ((real + imag) * cosine, (imag - real) * cosine)
    if 8 * index == 3 * size:
        return ((imag - real) * -cosine, (real + imag) * cosine)
    return (real * cosine - imag * sine, real * sine + imag * cosine)


def real_fft(values):
    size = len(values)
    if size == 2:
        return [(values[0] + values[1], None), (values[0] - values[1], None)]
    even = real_fft(values[0::2])
    odd = real_fft(values[1::2])
    half = size // 2
    out = [None] * (half + 1)
    out[0] = (even[0][0] + odd[0][0], None)
    out[half] = (even[0][0] - odd[0][0], None)
    quarter = size // 4
    out[quarter] = (even[quarter][0], -odd[quarter][0])
    for k in range(1, quarter):
        real, imag = turned(odd[k], k, size)
        out[k] = (even[k][0] + real, even[k][1] + imag)
        out[half - k] = (even[k][0] - real, imag - even[k][1])
    return out


def complex_fft(values):
    size = len(values)
    if size == 1:
        return values
    even = complex_fft(values[0::2])
    odd = complex_fft(values[1::2])
    half = size // 2
    out = [None] * size
    for k in range(half):
        real, imag = turned(odd[k], k, size)
        out[k] = (even[k][0] + real, even[k][1] + imag)
        out[k + half] = (even[k][0] - real, even[k][1] - imag)
    return out


def wave_matrix(angles):
    cosine, sine = np.cos(angles), np.sin(angles)
    return cosine, sine


def host_tables(extent):
    b = np.arange(LANES)[:, None]
    k = np.arange(LANES)[None, :]
    cosine, sine = wave_matrix(2 * np.pi * (b * k % LANES) / LANES)
    top = np.concatenate([cosine, -sine], 1)
    low = np.concatenate([sine, cosine], 1)
    natural = np.concatenate([top, low], 0)
    order = np.concatenate(
        [np.arange(HALF), LANES + np.arange(HALF), HALF + np.arange(HALF), LANES + HALF + np.arange(HALF)]
    )
    family = natural[:, order]
    first = np.zeros((2 * LANES, 2 * LANES))
    i = np.arange(HALF)[None, :]
    cosine, sine = wave_matrix(2 * np.pi * (b * i % LANES) / LANES)
    first[:LANES, :HALF] = cosine
    first[:LANES, HALF:LANES] = -sine
    first[:LANES, HALF] = 1.0 - 2.0 * (np.arange(LANES) % 2)
    freq = OUTER // 2 + OUTER * (HALF - 1 - i)
    cosine, sine = wave_matrix(2 * np.pi * (b * freq % extent) / extent)
    first[LANES:, LANES : LANES + HALF] = cosine
    first[LANES:, LANES + HALF :] = -sine
    return first, family, natural


def split_table(table):
    table = jnp.asarray(table, jnp.float32)
    high = table.astype(jnp.bfloat16)
    return high, (table - high.astype(jnp.float32)).astype(jnp.bfloat16)


def split_value(value):
    high = value.astype(jnp.bfloat16)
    return high, (value - high.astype(jnp.float32)).astype(jnp.bfloat16)


def dot_f32(left, right, dims=(((1,), (0,)), ((), ()))):
    return lax.dot_general(left, right, dims, preferred_element_type=jnp.float32)


def three_pass(value, table_high, table_low):
    high, low = split_value(value)
    return dot_f32(high, table_high) + (dot_f32(low, table_high) + dot_f32(high, table_low))


def row_kernel(map_ref, mask_ref, turn_ref, high_ref, low_ref, out0_ref, out1_ref, mid_ref):
    block = map_ref.shape[1]

    def tile(step, carry):
        start = pl.multiple_of(step * 8, 8)
        cells = []
        for a in range(OUTER):
            lanes = pl.ds(a * LANES, LANES)
            weight = mask_ref[pl.ds(start, 8), lanes].astype(jnp.float32)
            cells.append(map_ref[0, pl.ds(start, 8), lanes] * weight)
        waves = real_fft(cells)
        half = OUTER // 2
        mid_ref[0, pl.ds(start, 8), 0:LANES] = waves[0][0]
        mid_ref[0, pl.ds(start, 8), LANES : 2 * LANES] = waves[half][0]
        for k in range(1, half):
            real, imag = waves[k]
            cosine = turn_ref[0, k : k + 1, :]
            sine = turn_ref[1, k : k + 1, :]
            mid_ref[k, pl.ds(start, 8), 0:LANES] = real * cosine - imag * sine
            mid_ref[k, pl.ds(start, 8), LANES : 2 * LANES] = real * sine + imag * cosine
        return carry

    lax.fori_loop(0, block // 8, tile, 0)

    def family(k, carry):
        which = jnp.minimum(k, 1)
        value = three_pass(mid_ref[k], high_ref[which], low_ref[which])
        out0_ref[k] = value[:, :LANES]
        out1_ref[k] = value[:, LANES:]
        return carry

    lax.fori_loop(0, OUTER // 2, family, 0)


def bins_kernel(info_ref, bins_ref, flip_ref, out_ref, both_ref):
    step = pl.program_id(0)
    sub = bins_ref.shape[1]
    parity = info_ref[0]
    upper = info_ref[1]
    dests = out_ref.shape[0]
    width = out_ref.shape[3]
    for c in range(sub):
        kappa = step * sub + c
        mirrored = (OUTER - kappa) % OUTER
        turned_bins = bins_ref[:, c, :].astype(jnp.float32).T
        high = jnp.floor(turned_bins * 0.125)
        low = turned_bins - high * 8.0
        pair = jnp.concatenate([high.astype(jnp.bfloat16), low.astype(jnp.bfloat16)], 1)
        both_ref[0] = turned_bins
        both_ref[1] = dot_f32(pair, flip_ref[jnp.minimum(kappa, 1)])
        for dest in range(dests):
            fam = 2 * dest + parity
            zero = fam == 0
            col0 = jnp.where(zero & (upper == 1), OUTER // 2, fam)
            rev0 = jnp.where(zero & (upper == 1), 1, 0)
            col1 = jnp.where(zero, jnp.where(upper == 1, 0, OUTER // 2), OUTER - fam)
            rev1 = jnp.where(zero & (upper == 0), 0, 1)
            k0 = jnp.where(rev0 == 1, mirrored, kappa)
            k1 = jnp.where(rev1 == 1, mirrored, kappa)
            out_ref[dest, 0, k0] = both_ref[rev0, pl.ds(col0, width, stride=OUTER), :]
            out_ref[dest, 1, k1] = both_ref[rev1, pl.ds(col1, width, stride=OUTER), :]


def band_kernel(
    extent, nbins, chunk, info_ref, x_ref, bins0_ref, bins1_ref, turn_ref, high_ref, low_ref, fx_ref,
    sums_ref, edge_ref, mid_ref, power_ref, part_ref,
):
    offset = info_ref[0]
    flipped = info_ref[1]
    hollow = info_ref[2]
    local = x_ref.shape[2]
    per_slab = local // LANES
    lane8 = lax.broadcasted_iota(jnp.int32, (8, LANES), 1)
    left8 = lane8 < HALF

    def tile(step, carry):
        start = pl.multiple_of(step * 8, 8)
        cells = []
        for a in range(OUTER):
            rows = pl.ds((a % per_slab) * LANES + start, 8)
            q = x_ref[a // per_slab, 0, rows, :]
            u = x_ref[a // per_slab, 1, rows, :]
            real = jnp.where(left8, q, pltpu.roll(u, HALF, 1))
            imag = jnp.where(left8, pltpu.roll(q, HALF, 1), u)
            cells.append((real, imag))
        waves = complex_fft(cells)
        turns = {1: (turn_ref[0, pl.ds(start, 8), :], turn_ref[1, pl.ds(start, 8), :])}
        mid_ref[0, pl.ds(start, 8), :] = waves[0][0]
        mid_ref[0, pl.ds(LANES + start, 8), :] = waves[0][1]
        for k in range(1, OUTER):
            if k not in turns:
                (ar, ai), (br, bi) = turns[k // 2], turns[k - k // 2]
                turns[k] = (ar * br - ai * bi, ar * bi + ai * br)
            cosine, sine = turns[k]
            real, imag = waves[k]
            mid_ref[k, pl.ds(start, 8), :] = real * cosine - imag * sine
            mid_ref[k, pl.ds(LANES + start, 8), :] = real * sine + imag * cosine
        return carry

    lax.fori_loop(0, LANES // 8, tile, 0)

    fx = fx_ref[...]
    lane = lax.broadcasted_iota(jnp.int32, (HALF, LANES), 1)
    slot = lax.broadcasted_iota(jnp.int32, (HALF, LANES), 0)
    keep = jnp.where((slot == 0) & (hollow == 1), 0.0, 1.0)
    inv_area = 1.0 / (extent * extent)
    group_iota = lax.broadcasted_iota(jnp.int32, (GROUPS, LANES), 0).astype(jnp.float32).astype(jnp.bfloat16)
    low_iota = lax.broadcasted_iota(jnp.int32, (LOWS, LANES), 0).astype(jnp.float32).astype(jnp.bfloat16)
    width = bins0_ref.shape[3]
    one = jnp.ones((LOWS, LANES), jnp.bfloat16)
    none = jnp.zeros((LOWS, LANES), jnp.bfloat16)
    empty = jnp.zeros((GROUPS, LANES), jnp.bfloat16)
    unroll = 8

    def family(k, acc):
        spectrum = three_pass(mid_ref[k].T, high_ref[...], low_ref[...])
        if chunk == 0:
            edge_ref[k, 0:1, :] = spectrum[0:1, :]
            edge_ref[k, 1:2, :] = spectrum[HALF : HALF + 1, :]
        q_real, q_imag = spectrum[:HALF, :LANES], spectrum[:HALF, LANES:]
        u_real, u_imag = spectrum[HALF:, :LANES], spectrum[HALF:, LANES:]
        row = lane * OUTER + k
        fy = jnp.where(row >= extent // 2, row - extent, row).astype(jnp.float32)
        radius = jnp.maximum(fx * fx + fy * fy, 1.0)
        cos_twice = (fx * fx - fy * fy) / radius
        sin_twice = 2.0 * fx * fy / radius

        def powers(sine, which):
            e_real = cos_twice * q_real + sine * u_real
            e_imag = cos_twice * q_imag + sine * u_imag
            b_real = cos_twice * u_real - sine * q_real
            b_imag = cos_twice * u_imag - sine * q_imag
            power_ref[which, 0] = (e_real * e_real + e_imag * e_imag) * inv_area * keep
            power_ref[which, 1] = (b_real * b_real + b_imag * b_imag) * inv_area * keep
            power_ref[which, 2] = (e_real * b_real + e_imag * b_imag) * inv_area * keep

        other = jnp.where(k == 0, 1, 0)
        powers(sin_twice, jnp.where(k == 0, 1 - flipped, 0))

        @pl.when(k == 0)
        def _():
            powers(jnp.where(row == extent // 2, -sin_twice, sin_twice), flipped)

        for index, bins_ref in enumerate((bins0_ref, bins1_ref)):
            for source in range(bins_ref.shape[0]):
                value = bins_ref[source, 0, k]
                high = jnp.floor(value * (1.0 / LOWS))
                part_ref[index, 0, source * width : (source + 1) * width] = high
                part_ref[index, 1, source * width : (source + 1) * width] = value - high * LOWS

        def slots(step, acc):
            weighted, lows = [], []
            for inner in range(unroll):
                i = step * unroll + inner
                mirror = (offset - i) & (HALF - 1)
                for index, at, source in ((0, i, 0), (1, mirror, other)):
                    def line(ref, *where_):
                        return ref[where_ + (pl.ds(at, 1), slice(None))]
                    high = part_ref[index, 0, pl.ds(at, 1), :]
                    low = part_ref[index, 1, pl.ds(at, 1), :]
                    high = jnp.broadcast_to(high, (GROUPS, LANES)).astype(jnp.bfloat16)
                    low = jnp.broadcast_to(low, (LOWS, LANES)).astype(jnp.bfloat16)
                    hot = high == group_iota
                    column = []
                    for kind in range(3):
                        power = power_ref[source, kind, pl.ds(i, 1), :]
                        power = jnp.broadcast_to(power, (GROUPS, LANES)).astype(jnp.bfloat16)
                        column.append(jnp.where(hot, power, empty))
                    weighted.append(jnp.concatenate(column, 0))
                    lows.append(jnp.where(low == low_iota, one, none))
            return acc + dot_f32(
                jnp.concatenate(weighted, 1), jnp.concatenate(lows, 1), (((1,), (1,)), ((), ()))
            )

        return lax.fori_loop(0, HALF // unroll, slots, acc)

    sums_ref[...] = lax.fori_loop(0, OUTER, family, jnp.zeros((3 * GROUPS, LOWS), jnp.float32))


def vmem_spec(*block):
    if block:
        return pl.BlockSpec(*block)
    return pl.BlockSpec(memory_space=pltpu.VMEM)


def summed(array, axis):
    distance = 0
    while 1 << distance < lax.axis_size(axis):
        array = array + partner(array, axis, distance)
        distance += 1
    return array


def edge_sums(edge, bins_left, bins_right, extent):
    flat = edge.transpose(1, 2, 0).reshape(2, 2, extent)
    back = jnp.roll(flat[:, :, ::-1], 1, axis=2)
    q_real, q_imag, u_real, u_imag = [
        jnp.stack(pair)
        for m in range(2)
        for pair in (
            (0.5 * (flat[m, 0] + back[m, 0]), 0.5 * (flat[m, 1] + back[m, 1])),
            (0.5 * (flat[m, 1] - back[m, 1]), 0.5 * (back[m, 0] - flat[m, 0])),
        )
    ]
    freq_y = signed_float(lax.iota(jnp.int32, extent), extent)[None, :]
    freq_x = jnp.array([0.0, -extent // 2], jnp.float32)[:, None]
    left = bins_left.T.reshape(extent)
    right = jnp.roll(bins_right.T.reshape(extent)[::-1], 1)
    bins = jnp.stack([left, right]).astype(jnp.int32)
    return band_terms((q_real, q_imag, u_real, u_imag), freq_y, freq_x, bins, NBINS, extent)


def on_device_fast(maps, mask, bins):
    extent = bins.shape[0]
    columns = bins.shape[1]
    count = maps.shape[1]
    slabs = lax.axis_size("rows")
    reps = lax.axis_size("rep")
    slab_index = lax.axis_index("rows")
    member = lax.axis_index("rep")
    pair_bit = member % 2
    half_slabs = slabs // 2
    first, family, natural = host_tables(extent)
    row_high, row_low = split_table(np.stack([first, family]))
    col_high, col_low = split_table(natural)

    flips = np.zeros((2, 2 * LANES, LANES))
    for k in range(LANES):
        flips[0, k, -k % LANES] = 8.0
        flips[0, LANES + k, -k % LANES] = 1.0
        flips[1, k, LANES - 1 - k] = 8.0
        flips[1, LANES + k, LANES - 1 - k] = 1.0
    info = jnp.stack([pair_bit, (slab_index >= half_slabs).astype(jnp.int32)])
    sub = 8
    width = columns // OUTER
    sent_bins = pl.pallas_call(
        bins_kernel,
        grid=(OUTER // sub,),
        in_specs=[
            pl.BlockSpec(memory_space=pltpu.SMEM),
            pl.BlockSpec((LANES, sub, columns), lambda i: (0, i, 0)),
            pl.BlockSpec((2, 2 * LANES, LANES), lambda i: (0, 0, 0)),
        ],
        out_specs=pl.BlockSpec((slabs, 2, OUTER, width, LANES), lambda i: (0, 0, 0, 0, 0)),
        out_shape=jax.ShapeDtypeStruct((slabs, 2, OUTER, width, LANES), jnp.float32),
        scratch_shapes=[pltpu.VMEM((2, columns, LANES), jnp.float32)],
        name="bins_prep",
    )(info, bins.reshape(LANES, OUTER, columns), jnp.asarray(flips, jnp.bfloat16))
    got_bins = lax.all_to_all(sent_bins, "rows", split_axis=0, concat_axis=0, tiled=True)

    block = min(LANES, count)
    k1 = np.arange(OUTER // 2)[:, None]
    angles = 2 * np.pi * (k1 * np.arange(LANES)[None, :] % extent) / extent
    turns = jnp.asarray(np.stack([np.cos(angles), -np.sin(angles)]), jnp.float32)
    table_spec = pl.BlockSpec((2, 2 * LANES, 2 * LANES), lambda i: (0, 0, 0))
    piece = jax.ShapeDtypeStruct((2 * slabs, count, LANES), jnp.float32)
    piece_spec = pl.BlockSpec((2 * slabs, block, LANES), lambda i: (0, i, 0))
    pieces = pl.pallas_call(
        row_kernel,
        grid=(count // block,),
        in_specs=[
            pl.BlockSpec((1, block, extent), lambda i: (0, i, 0)),
            pl.BlockSpec((block, extent), lambda i: (i, 0)),
            pl.BlockSpec(turns.shape, lambda i: (0, 0, 0)),
            table_spec,
            table_spec,
        ],
        out_specs=[piece_spec, piece_spec],
        out_shape=[piece, piece],
        scratch_shapes=[pltpu.VMEM((OUTER // 2, block, 2 * LANES), jnp.float32)],
        name="row_fft",
    )(maps, mask, turns, row_high, row_low)

    groups = [
        [row * reps + z for row in range(slabs) for z in (2 * sky, 2 * sky + 1)]
        for sky in range(reps // 2)
    ]
    fam = 2 * slab_index + pair_bit
    angles = 2 * np.pi * np.arange(LANES) / extent
    spin = np.stack([np.cos(angles), -np.sin(angles)])[:, :, None]
    spin = jnp.asarray(np.broadcast_to(spin, (2, LANES, LANES)), jnp.float32)
    slots = lax.iota(jnp.int32, HALF)
    total = None
    for chunk in range(2):
        got = lax.all_to_all(
            pieces[chunk], ("rows", "rep"), split_axis=0, concat_axis=0, tiled=True,
            axis_index_groups=groups,
        ).reshape(slabs, 2, count, LANES)
        first_col = OUTER * slots if chunk == 0 else OUTER // 2 + OUTER * (HALF - 1 - slots)
        col = jnp.where(fam == 0, first_col, fam + OUTER * (slots + HALF * chunk))
        fx = jnp.broadcast_to(signed_float(col, extent)[:, None], (HALF, LANES))
        zero = (fam == 0).astype(jnp.int32)
        if chunk == 0:
            info = jnp.stack([HALF - 1 + zero, jnp.int32(1), zero])
        else:
            info = jnp.stack([jnp.int32(HALF - 1), 1 - zero, jnp.int32(0)])
        bin_block = (half_slabs, 1, OUTER, width, LANES)
        sums, edge = pl.pallas_call(
            functools.partial(band_kernel, extent, NBINS, chunk),
            grid=(1,),
            in_specs=[
                pl.BlockSpec(memory_space=pltpu.SMEM),
                pl.BlockSpec(got.shape, lambda i: (0, 0, 0, 0)),
                pl.BlockSpec(bin_block, lambda i, at=chunk: (at, 0, 0, 0, 0)),
                pl.BlockSpec(bin_block, lambda i, at=1 - chunk: (at, 1, 0, 0, 0)),
                pl.BlockSpec(spin.shape, lambda i: (0, 0, 0)),
                pl.BlockSpec(col_high.shape, lambda i: (0, 0)),
                pl.BlockSpec(col_low.shape, lambda i: (0, 0)),
                pl.BlockSpec(fx.shape, lambda i: (0, 0)),
            ],
            out_specs=[
                pl.BlockSpec((3 * GROUPS, LOWS), lambda i: (0, 0)),
                pl.BlockSpec((OUTER, 2, 2 * LANES), lambda i: (0, 0, 0)),
            ],
            out_shape=[
                jax.ShapeDtypeStruct((3 * GROUPS, LOWS), jnp.float32),
                jax.ShapeDtypeStruct((OUTER, 2, 2 * LANES), jnp.float32),
            ],
            scratch_shapes=[
                pltpu.VMEM((OUTER, 2 * LANES, LANES), jnp.float32),
                pltpu.VMEM((2, 3, HALF, LANES), jnp.float32),
                pltpu.VMEM((2, 2, HALF, LANES), jnp.float32),
            ],
            compiler_params=pltpu.CompilerParams(vmem_limit_bytes=48 * 2**20),
            name="band_sums",
        )(info, got, got_bins, got_bins, spin, col_high, col_low, fx)
        total = sums if total is None else total + sums
        if chunk == 0:
            special = edge_sums(edge, got_bins[0, 0, :, 0], got_bins[half_slabs, 1, :, 0], extent)
            special = jnp.where(fam == 0, special, 0.0)
    partial_sums = total.reshape(3, NBINS) + special
    auto = NBINS / (extent * extent)
    cross = math.sqrt(auto)
    factors = jnp.array([auto, auto, cross], jnp.float32)[:, None]
    own = summed(partial_sums, "rows")
    own = (own + partner(own, "rep", 0)) * factors
    skies = [own]
    distance = 1
    while 1 << distance < reps:
        skies = skies + [partner(sky, "rep", distance) for sky in skies]
        distance += 1
    stacked = jnp.stack(skies)
    order = lax.iota(jnp.int32, len(skies)) ^ (member // 2)
    return jnp.take(stacked, order, axis=0) if len(skies) > 2 else jnp.where(
        member // 2 == 0, stacked, stacked[::-1]
    )


def solution(mesh):
    in_specs = (P("rep", "rows", None), P("rows", None), P(None, "rows"))
    out_specs = P()

    def on_any(maps, mask, bins):
        extent = bins.shape[0]
        families = 2 * lax.axis_size("rows")
        if extent == OUTER * LANES and families == OUTER // 2 and NBINS == GROUPS * LOWS:
            return on_device_fast(maps, mask, bins)
        return on_device(maps, mask, bins)

    return jax.shard_map(
        on_any, mesh=mesh, in_specs=in_specs, out_specs=out_specs, check_vma=False
    )
```

```python
import functools
import math

import jax
import jax.numpy as jnp
import numpy as np
from jax import lax
from jax.experimental import pallas as pl
from jax.experimental.pallas import tpu as pltpu
from jax.sharding import PartitionSpec as P

NBINS = 1024


precise = lax.Precision.HIGHEST


def partner(array, axis, distance):
    return lax.ppermute(array, axis, [(i, i ^ 1 << distance) for i in range(lax.axis_size(axis))])


def dft_table(count_a, count_b, period):
    first = lax.iota(jnp.int32, count_a)[:, None]
    second = lax.iota(jnp.int32, count_b)[None, :]
    angles = (first * second % period).astype(jnp.float32) * (2.0 * math.pi / period)
    return (jnp.cos(angles), -jnp.sin(angles))


def split_length(length):
    outer_len = 2 ** ((length.bit_length() - 1) // 2)
    return (outer_len, length // outer_len)


def complex_apply(form, real_part, imag_part, table_cos, table_sin):

    def product(left, right):
        return jnp.einsum(form, left, right, precision=precise)

    return (
        product(real_part, table_cos) - product(imag_part, table_sin),
        product(real_part, table_sin) + product(imag_part, table_cos),
    )


def twiddled(real_part, imag_part, table_cos, table_sin):
    return (
        real_part * table_cos - imag_part * table_sin,
        real_part * table_sin + imag_part * table_cos,
    )


def row_transform(values):
    count, length = values.shape
    outer_len, inner_len = split_length(length)
    outer_cos, outer_sin = dft_table(outer_len, outer_len, outer_len)
    inner_cos, inner_sin = dft_table(inner_len, inner_len, inner_len)
    turn_cos, turn_sin = dft_table(outer_len, inner_len, length)
    shaped = values.reshape(count, outer_len, inner_len)
    first_real = jnp.einsum("yan,ak->ykn", shaped, outer_cos, precision=precise)
    first_imag = jnp.einsum("yan,ak->ykn", shaped, outer_sin, precision=precise)
    mid_real, mid_imag = twiddled(first_real, first_imag, turn_cos, turn_sin)
    last_real, last_imag = complex_apply("ykn,nm->ymk", mid_real, mid_imag, inner_cos, inner_sin)
    return (last_real.reshape(count, length), last_imag.reshape(count, length))


def column_transform(pieces):
    real_part, imag_part = pieces
    length, groups, width = real_part.shape
    outer_len, inner_len = split_length(length)
    outer_cos, outer_sin = dft_table(outer_len, outer_len, outer_len)
    inner_cos, inner_sin = dft_table(inner_len, inner_len, inner_len)
    turn_cos, turn_sin = dft_table(outer_len, inner_len, length)
    shaped_real = real_part.reshape(outer_len, inner_len, groups, width)
    shaped_imag = imag_part.reshape(outer_len, inner_len, groups, width)
    first_real, first_imag = complex_apply(
        "anbc,ak->knbc", shaped_real, shaped_imag, outer_cos, outer_sin
    )
    mid_real, mid_imag = twiddled(
        first_real, first_imag, turn_cos[:, :, None, None], turn_sin[:, :, None, None]
    )
    last_real, last_imag = complex_apply("knbc,nm->mkbc", mid_real, mid_imag, inner_cos, inner_sin)
    return (last_real.reshape(length, groups, width), last_imag.reshape(length, groups, width))


def signed_float(indices, extent):
    return jnp.where(indices >= extent // 2, indices - extent, indices).astype(jnp.float32)


def band_terms(fields, freq_y, freq_x, bin_block, nbins_count, extent):
    q_real, q_imag, u_real, u_imag = fields
    radius = jnp.maximum(freq_x * freq_x + freq_y * freq_y, 1.0)
    cos_twice = (freq_x * freq_x - freq_y * freq_y) / radius
    sin_twice = 2.0 * freq_x * freq_y / radius
    e_real = cos_twice * q_real + sin_twice * u_real
    e_imag = cos_twice * q_imag + sin_twice * u_imag
    b_real = -sin_twice * q_real + cos_twice * u_real
    b_imag = -sin_twice * q_imag + cos_twice * u_imag
    inv_area = 1.0 / (extent * extent)
    powers = jnp.stack(
        [
            (e_real * e_real + e_imag * e_imag) * inv_area,
            (b_real * b_real + b_imag * b_imag) * inv_area,
            (e_real * b_real + e_imag * b_imag) * inv_area,
        ]
    ).astype(jnp.bfloat16)
    bit_count = nbins_count.bit_length() - 1
    high_count = 2 ** max(bit_count // 2 - 1, 0)
    low_count = nbins_count // high_count
    high_part = bin_block // low_count
    low_part = bin_block % low_count
    high_hot = (high_part[None] == lax.iota(jnp.int32, high_count)[:, None, None]).astype(
        jnp.bfloat16
    )
    weighted = (powers[:, None] * high_hot[None]).reshape(3 * high_count, -1)
    low_hot = (low_part[None] == lax.iota(jnp.int32, low_count)[:, None, None]).astype(jnp.bfloat16)
    low_hot = low_hot.reshape(low_count, -1)
    sums = lax.dot_general(
        weighted, low_hot, (((1,), (1,)), ((), ())), preferred_element_type=jnp.float32
    )
    return sums.reshape(3, nbins_count)


def on_device(maps, mask, bins):
    extent = bins.shape[0]
    columns = bins.shape[1]
    count = maps.shape[1]
    slab_index = lax.axis_index("rows")
    member = lax.axis_index("rep")
    pair_bit = member % 2
    field = maps[0] * mask.astype(jnp.float32)
    row_real, row_imag = row_transform(field)
    half_rows = extent // 2
    slabs = (
        row_real.reshape(count, extent // columns, columns),
        row_imag.reshape(count, extent // columns, columns),
    )
    spec_real, spec_imag = column_transform(
        (
            lax.all_to_all(slabs[0], "rows", split_axis=1, concat_axis=0, tiled=True),
            lax.all_to_all(slabs[1], "rows", split_axis=1, concat_axis=0, tiled=True),
        )
    )
    spec_real = spec_real.reshape(extent, columns)
    spec_imag = spec_imag.reshape(extent, columns)
    kept_real = lax.dynamic_slice_in_dim(spec_real, pair_bit * half_rows, half_rows, 0)
    kept_imag = lax.dynamic_slice_in_dim(spec_imag, pair_bit * half_rows, half_rows, 0)
    sent_real = lax.dynamic_slice_in_dim(spec_real, (1 - pair_bit) * half_rows, half_rows, 0)
    sent_imag = lax.dynamic_slice_in_dim(spec_imag, (1 - pair_bit) * half_rows, half_rows, 0)
    got_real, got_imag = partner((sent_real, sent_imag), "rep", 0)
    is_first = pair_bit == 0
    fields = (
        jnp.where(is_first, kept_real, got_real),
        jnp.where(is_first, kept_imag, got_imag),
        jnp.where(is_first, got_real, kept_real),
        jnp.where(is_first, got_imag, kept_imag),
    )
    own_bins = lax.dynamic_slice_in_dim(bins, pair_bit * half_rows, half_rows, 0)

    def frequency_of(offset, height):
        rows_here = lax.iota(jnp.int32, height)[:, None] + offset + pair_bit * half_rows
        cols_here = lax.iota(jnp.int32, columns)[None, :] + slab_index * columns
        return (rows_here, cols_here)

    block = min(256, half_rows)
    blocks = half_rows // block
    stacked = tuple((part.reshape(blocks, block, columns) for part in fields))
    bin_blocks = own_bins.reshape(blocks, block, columns)

    def accumulate(running, items):
        block_index, parts, bin_block = items
        rows_here, cols_here = frequency_of(block_index * block, block)
        term = band_terms(
            parts,
            signed_float(rows_here, extent),
            signed_float(cols_here, extent),
            bin_block,
            NBINS,
            extent,
        )
        return (running + term, None)

    partial_sums, _ = lax.scan(
        accumulate,
        jnp.zeros((3, NBINS), jnp.float32),
        (lax.iota(jnp.int32, blocks), stacked, bin_blocks),
    )
    sims_count = lax.axis_size("rep") // 2
    slot = (lax.iota(jnp.int32, sims_count) == member // 2).astype(jnp.float32)[:, None, None]
    totals = lax.psum(slot * partial_sums[None], ("rows", "rep"))
    auto = NBINS / (extent * extent)
    cross = math.sqrt(auto)
    factors = jnp.array([auto, auto, cross], jnp.float32)[None, :, None]
    return totals * factors


LANES = 128
OUTER = 32
HALF = LANES // 2
SUB = LANES // 4
GROUPS = 16
LOWS = 64


def fft_wave(index, size):
    return (math.cos(2 * math.pi * index / size), -math.sin(2 * math.pi * index / size))


def turned(value, index, size):
    real, imag = value
    if index == 0:
        return value
    if 4 * index == size:
        return (imag, -real)
    cosine, sine = fft_wave(index, size)
    if 8 * index == size:
        return ((real + imag) * cosine, (imag - real) * cosine)
    if 8 * index == 3 * size:
        return ((imag - real) * -cosine, (real + imag) * cosine)
    return (real * cosine - imag * sine, real * sine + imag * cosine)


def real_fft(values):
    size = len(values)
    if size == 2:
        return [(values[0] + values[1], None), (values[0] - values[1], None)]
    even = real_fft(values[0::2])
    odd = real_fft(values[1::2])
    half = size // 2
    out = [None] * (half + 1)
    out[0] = (even[0][0] + odd[0][0], None)
    out[half] = (even[0][0] - odd[0][0], None)
    quarter = size // 4
    out[quarter] = (even[quarter][0], -odd[quarter][0])
    for k in range(1, quarter):
        real, imag = turned(odd[k], k, size)
        out[k] = (even[k][0] + real, even[k][1] + imag)
        out[half - k] = (even[k][0] - real, imag - even[k][1])
    return out


def complex_fft(values):
    size = len(values)
    if size == 1:
        return values
    even = complex_fft(values[0::2])
    odd = complex_fft(values[1::2])
    half = size // 2
    out = [None] * size
    for k in range(half):
        real, imag = turned(odd[k], k, size)
        out[k] = (even[k][0] + real, even[k][1] + imag)
        out[k + half] = (even[k][0] - real, even[k][1] - imag)
    return out


def wave_matrix(angles):
    cosine, sine = np.cos(angles), np.sin(angles)
    return cosine, sine


def host_tables(extent):
    b = np.arange(LANES)[:, None]
    k = np.arange(LANES)[None, :]
    cosine, sine = wave_matrix(2 * np.pi * (b * k % LANES) / LANES)
    natural = np.concatenate(
        [np.concatenate([cosine, -sine], 1), np.concatenate([sine, cosine], 1)], 0
    )
    first = np.zeros((2 * LANES, 2 * LANES))
    first[:LANES, :HALF] = cosine[:, :HALF]
    first[:LANES, LANES : LANES + HALF] = -sine[:, :HALF]
    first[:LANES, LANES] = 1.0 - 2.0 * (np.arange(LANES) % 2)
    freq = OUTER // 2 + OUTER * (HALF - 1 - np.arange(HALF)[None, :])
    cosine, sine = wave_matrix(2 * np.pi * (b * freq % extent) / extent)
    first[LANES:, HALF:LANES] = cosine
    first[LANES:, LANES + HALF :] = -sine
    order = np.concatenate(
        [part + SUB * s + np.arange(SUB) for s in range(LANES // SUB) for part in (0, LANES)]
    )
    rows = np.concatenate([part + HALF * h + np.arange(HALF) for h in range(2) for part in (0, LANES)])
    return first[:, order], natural[:, order], natural[rows]


def split_table(table):
    table = jnp.asarray(table, jnp.float32)
    high = table.astype(jnp.bfloat16)
    return high, (table - high.astype(jnp.float32)).astype(jnp.bfloat16)


def split_value(value):
    high = value.astype(jnp.bfloat16)
    return high, (value - high.astype(jnp.float32)).astype(jnp.bfloat16)


def dot_f32(left, right, dims=(((1,), (0,)), ((), ()))):
    return lax.dot_general(left, right, dims, preferred_element_type=jnp.float32)


def three_pass(value, table_high, table_low):
    high, low = split_value(value)
    return dot_f32(high, table_high) + (dot_f32(low, table_high) + dot_f32(high, table_low))


def row_kernel(
    map_ref, mask_ref, turn_ref, high_ref, low_ref, first_ref, second_ref, mid_ref
):
    block = map_ref.shape[1]
    left = lax.broadcasted_iota(jnp.int32, (block // 2, LANES), 1) < HALF

    def tile(step, carry):
        start = pl.multiple_of(step * 8, 8)
        cells = []
        for a in range(OUTER):
            lanes = pl.ds(a * LANES, LANES)
            weight = mask_ref[pl.ds(start, 8), lanes].astype(jnp.float32)
            cells.append(map_ref[0, pl.ds(start, 8), lanes] * weight)
        waves = real_fft(cells)
        half = OUTER // 2
        mid_ref[0, pl.ds(start, 8), 0:LANES] = waves[0][0]
        mid_ref[0, pl.ds(start, 8), LANES : 2 * LANES] = waves[half][0]
        for k in range(1, half):
            real, imag = waves[k]
            cosine = turn_ref[0, k : k + 1, :]
            sine = turn_ref[1, k : k + 1, :]
            mid_ref[k, pl.ds(start, 8), 0:LANES] = real * cosine - imag * sine
            mid_ref[k, pl.ds(start, 8), LANES : 2 * LANES] = real * sine + imag * cosine
        return carry

    lax.fori_loop(0, block // 8, tile, 0)

    def family(k, carry):
        which = jnp.minimum(k, 1)
        value = three_pass(mid_ref[k], high_ref[which], low_ref[which])
        subs = []
        for lanes in (slice(0, LANES), slice(LANES, 2 * LANES)):
            top, low = value[: block // 2, lanes], value[block // 2 :, lanes]
            subs.append(jnp.where(left, top, pltpu.roll(low, HALF, 1)))
            subs.append(jnp.where(left, pltpu.roll(top, HALF, 1), low))
        for index in range(2):
            first_ref[k, index] = subs[index]
            second_ref[k, index] = subs[2 + index]
        return carry

    lax.fori_loop(0, OUTER // 2, family, 0)


def bins_kernel(info_ref, bins_ref, flip_ref, out_ref, turn_ref):
    step = pl.program_id(0)
    sub = bins_ref.shape[1]
    parity = info_ref[0]
    upper = info_ref[1]
    dests = out_ref.shape[0]
    width = out_ref.shape[3]
    zero = parity == 0
    high_side = upper == 1
    for c in range(sub):
        kappa = step * sub + c
        mirrored = (OUTER - kappa) % OUTER
        turn_ref[c % 2] = bins_ref[:, c, :].astype(jnp.float32).T

        def column(at):
            return turn_ref[c % 2, pl.ds(at, width, stride=OUTER), :]

        ahead = [column(jnp.where(zero & high_side, OUTER // 2, parity))]
        back = [column(jnp.where(zero, jnp.where(high_side, 0, OUTER // 2), OUTER - parity))]
        for dest in range(1, dests):
            ahead.append(column(2 * dest + parity))
            back.append(column(OUTER - 2 * dest - parity))
        mixed = jnp.concatenate([ahead[0]] + back, 0)
        high = jnp.floor(mixed * 0.125)
        pair = jnp.concatenate([high.astype(jnp.bfloat16), (mixed - high * 8.0).astype(jnp.bfloat16)], 1)
        flipped = dot_f32(pair, flip_ref[jnp.minimum(kappa, 1)])
        turn0 = zero & high_side
        turn1 = jnp.logical_not(zero & jnp.logical_not(high_side))
        out_ref[0, 0, jnp.where(turn0, mirrored, kappa)] = jnp.where(turn0, flipped[:width], ahead[0])
        out_ref[0, 1, jnp.where(turn1, mirrored, kappa)] = jnp.where(
            turn1, flipped[width : 2 * width], back[0]
        )
        for dest in range(1, dests):
            out_ref[dest, 0, kappa] = ahead[dest]
            out_ref[dest, 1, mirrored] = flipped[(dest + 1) * width : (dest + 2) * width]


def band_kernel(
    extent, with_edge, info_ref, x_ref, bins0_ref, bins1_ref, turn_ref, high_ref, low_ref,
    fx_ref, *refs,
):
    if with_edge:
        sums_ref, edge_ref, mid_ref, power_ref, part_ref = refs
    else:
        sums_ref, mid_ref, power_ref, part_ref = refs
    sub = pl.program_id(0)
    offset = info_ref[0]
    flipped = info_ref[1]
    hollow = (info_ref[2] == 1) & (sub == 0)
    per_slab = x_ref.shape[3] // HALF
    even8 = lax.broadcasted_iota(jnp.int32, (8, LANES), 1) % HALF < SUB

    def tile(step, carry):
        start = pl.multiple_of(step * 8, 8)
        cells = []
        for a in range(OUTER):
            rows = pl.ds((a % per_slab) * HALF + start, 8)
            q = x_ref[a // per_slab, 0, 0, rows, :]
            u = x_ref[a // per_slab, 1, 0, rows, :]
            real = jnp.where(even8, q, pltpu.roll(u, SUB, 1))
            imag = jnp.where(even8, pltpu.roll(q, LANES - SUB, 1), u)
            cells.append((real, imag))
        waves = complex_fft(cells)
        turns = {1: (turn_ref[0, pl.ds(start, 8), :], turn_ref[1, pl.ds(start, 8), :])}
        mid_ref[0, pl.ds(start, 8), :] = waves[0][0]
        mid_ref[0, pl.ds(HALF + start, 8), :] = waves[0][1]
        for k in range(1, OUTER):
            if k not in turns:
                (ar, ai), (br, bi) = turns[k // 2], turns[k - k // 2]
                turns[k] = (ar * br - ai * bi, ar * bi + ai * br)
            cosine, sine = turns[k]
            real, imag = waves[k]
            mid_ref[k, pl.ds(start, 8), :] = real * cosine - imag * sine
            mid_ref[k, pl.ds(HALF + start, 8), :] = real * sine + imag * cosine
        return carry

    lax.fori_loop(0, HALF // 8, tile, 0)

    fx = fx_ref[0]
    lane = lax.broadcasted_iota(jnp.int32, (SUB, LANES), 1)
    slot = lax.broadcasted_iota(jnp.int32, (SUB, LANES), 0)
    keep = jnp.where((slot == 0) & hollow, 0.0, 1.0)
    inv_area = 1.0 / (extent * extent)
    group_iota = lax.broadcasted_iota(jnp.int32, (GROUPS, LANES), 0).astype(jnp.float32).astype(jnp.bfloat16)
    low_iota = lax.broadcasted_iota(jnp.int32, (LOWS, LANES), 0).astype(jnp.float32).astype(jnp.bfloat16)
    width = bins0_ref.shape[3]
    near = SUB // width
    one = jnp.ones((LOWS, LANES), jnp.bfloat16)
    none = jnp.zeros((LOWS, LANES), jnp.bfloat16)
    empty = jnp.zeros((GROUPS, LANES), jnp.bfloat16)
    begin0 = sub * near
    begin1 = (1 - sub) * near

    def pair(step, acc):
        turned_rows = []
        for member in range(2):
            flat = mid_ref[2 * step + member].T
            turned_rows.append(jnp.concatenate([flat[:HALF], flat[HALF:]], 1))
        spectra = three_pass(jnp.concatenate(turned_rows, 0), high_ref[...], low_ref[...])
        weighted, lows = [], []
        for member in range(2):
            k = 2 * step + member
            spectrum = spectra[member * HALF : (member + 1) * HALF]
            if with_edge:
                edge_ref[sub, k, 0:1, :] = spectrum[0:1, :]
                edge_ref[sub, k, 1:2, :] = spectrum[SUB : SUB + 1, :]
            q_real, q_imag = spectrum[:SUB, :LANES], spectrum[:SUB, LANES:]
            u_real, u_imag = spectrum[SUB:, :LANES], spectrum[SUB:, LANES:]
            row = lane * OUTER + k
            fy = jnp.where(row >= extent // 2, row - extent, row).astype(jnp.float32)
            radius = jnp.maximum(fx * fx + fy * fy, 1.0)
            cos_twice = (fx * fx - fy * fy) / radius
            sin_twice = 2.0 * fx * fy / radius

            def powers(sine, which):
                e_real = cos_twice * q_real + sine * u_real
                e_imag = cos_twice * q_imag + sine * u_imag
                b_real = cos_twice * u_real - sine * q_real
                b_imag = cos_twice * u_imag - sine * q_imag
                power_ref[member, which, 0] = (e_real * e_real + e_imag * e_imag) * inv_area * keep
                power_ref[member, which, 1] = (b_real * b_real + b_imag * b_imag) * inv_area * keep
                power_ref[member, which, 2] = (e_real * b_real + e_imag * b_imag) * inv_area * keep

            other = 0
            if member == 0:
                other = jnp.where(k == 0, 1, 0)
                powers(sin_twice, jnp.where(k == 0, 1 - flipped, 0))

                @pl.when(k == 0)
                def _():
                    powers(jnp.where(row == extent // 2, -sin_twice, sin_twice), flipped)

            else:
                powers(sin_twice, 0)

            for index, (bins_ref, begin, count) in enumerate(
                ((bins0_ref, begin0, near), (bins1_ref, begin1, near + 1))
            ):
                for source in range(count):
                    at = jnp.minimum(begin + source, bins_ref.shape[0] - 1)
                    value = bins_ref[at, 0, k]
                    high = jnp.floor(value * (1.0 / LOWS))
                    rows = slice(source * width, (source + 1) * width)
                    part_ref[member, index, 0, rows] = high
                    part_ref[member, index, 1, rows] = value - high * LOWS

            for i in range(SUB):
                mirror = offset - HALF + SUB - i
                for index, at, source in ((0, i, 0), (1, mirror, other)):
                    high = part_ref[member, index, 0, pl.ds(at, 1), :]
                    low = part_ref[member, index, 1, pl.ds(at, 1), :]
                    high = jnp.broadcast_to(high, (GROUPS, LANES)).astype(jnp.bfloat16)
                    low = jnp.broadcast_to(low, (LOWS, LANES)).astype(jnp.bfloat16)
                    hot = high == group_iota
                    column = []
                    for kind in range(3):
                        power = power_ref[member, source, kind, pl.ds(i, 1), :]
                        power = jnp.broadcast_to(power, (GROUPS, LANES)).astype(jnp.bfloat16)
                        column.append(jnp.where(hot, power, empty))
                    weighted.append(jnp.concatenate(column, 0))
                    lows.append(jnp.where(low == low_iota, one, none))
        return acc + dot_f32(
            jnp.concatenate(weighted, 1), jnp.concatenate(lows, 1), (((1,), (1,)), ((), ()))
        )

    sums_ref[0] = lax.fori_loop(0, OUTER // 2, pair, jnp.zeros((3 * GROUPS, LOWS), jnp.float32))


def summed(array, axis):
    distance = 0
    while 1 << distance < lax.axis_size(axis):
        array = array + partner(array, axis, distance)
        distance += 1
    return array


def edge_sums(edge, bins_left, bins_right, extent):
    flat = edge.transpose(1, 2, 0).reshape(2, 2, extent)
    back = jnp.roll(flat[:, :, ::-1], 1, axis=2)
    q_real, q_imag, u_real, u_imag = [
        jnp.stack(pair)
        for m in range(2)
        for pair in (
            (0.5 * (flat[m, 0] + back[m, 0]), 0.5 * (flat[m, 1] + back[m, 1])),
            (0.5 * (flat[m, 1] - back[m, 1]), 0.5 * (back[m, 0] - flat[m, 0])),
        )
    ]
    freq_y = signed_float(lax.iota(jnp.int32, extent), extent)[None, :]
    freq_x = jnp.array([0.0, -extent // 2], jnp.float32)[:, None]
    left = bins_left.T.reshape(extent)
    right = jnp.roll(bins_right.T.reshape(extent)[::-1], 1)
    bins = jnp.stack([left, right]).astype(jnp.int32)
    return band_terms((q_real, q_imag, u_real, u_imag), freq_y, freq_x, bins, NBINS, extent)


def on_device_fast(maps, mask, bins):
    extent = bins.shape[0]
    columns = bins.shape[1]
    count = maps.shape[1]
    slabs = lax.axis_size("rows")
    reps = lax.axis_size("rep")
    slab_index = lax.axis_index("rows")
    member = lax.axis_index("rep")
    pair_bit = member % 2
    half_slabs = slabs // 2
    first, family, natural = host_tables(extent)
    row_high, row_low = split_table(np.stack([first, family]))
    col_high, col_low = split_table(natural)

    flips = np.zeros((2, 2 * LANES, LANES))
    for k in range(LANES):
        flips[0, k, -k % LANES] = 8.0
        flips[0, LANES + k, -k % LANES] = 1.0
        flips[1, k, LANES - 1 - k] = 8.0
        flips[1, LANES + k, LANES - 1 - k] = 1.0
    info = jnp.stack([pair_bit, (slab_index >= half_slabs).astype(jnp.int32)])
    sub = 8
    width = columns // OUTER
    sent_bins = pl.pallas_call(
        bins_kernel,
        grid=(OUTER // sub,),
        in_specs=[
            pl.BlockSpec(memory_space=pltpu.SMEM),
            pl.BlockSpec((LANES, sub, columns), lambda i: (0, i, 0)),
            pl.BlockSpec((2, 2 * LANES, LANES), lambda i: (0, 0, 0)),
        ],
        out_specs=pl.BlockSpec((slabs, 2, OUTER, width, LANES), lambda i: (0, 0, 0, 0, 0)),
        out_shape=jax.ShapeDtypeStruct((slabs, 2, OUTER, width, LANES), jnp.float32),
        scratch_shapes=[pltpu.VMEM((2, columns, LANES), jnp.float32)],
        name="bins_prep",
    )(info, bins.reshape(LANES, OUTER, columns), jnp.asarray(flips, jnp.bfloat16))
    got_bins = lax.all_to_all(sent_bins, "rows", split_axis=0, concat_axis=0, tiled=True)

    block = min(LANES, count)
    k1 = np.arange(OUTER // 2)[:, None]
    angles = 2 * np.pi * (k1 * np.arange(LANES)[None, :] % extent) / extent
    turns = jnp.asarray(np.stack([np.cos(angles), -np.sin(angles)]), jnp.float32)
    table_spec = pl.BlockSpec((2, 2 * LANES, 2 * LANES), lambda i: (0, 0, 0))
    piece = jax.ShapeDtypeStruct((2 * slabs, 2, count // 2, LANES), jnp.float32)
    piece_spec = pl.BlockSpec((2 * slabs, 2, block // 2, LANES), lambda i: (0, 0, i, 0))
    pieces = pl.pallas_call(
        row_kernel,
        grid=(count // block,),
        in_specs=[
            pl.BlockSpec((1, block, extent), lambda i: (0, i, 0)),
            pl.BlockSpec((block, extent), lambda i: (i, 0)),
            pl.BlockSpec(turns.shape, lambda i: (0, 0, 0)),
            table_spec,
            table_spec,
        ],
        out_specs=[piece_spec, piece_spec],
        out_shape=[piece, piece],
        scratch_shapes=[pltpu.VMEM((OUTER // 2, block, 2 * LANES), jnp.float32)],
        name="row_fft",
    )(maps, mask, turns, row_high, row_low)

    groups = [
        [row * reps + z for row in range(slabs) for z in (2 * sky, 2 * sky + 1)]
        for sky in range(reps // 2)
    ]
    fam = 2 * slab_index + pair_bit
    angles = np.arange(HALF)[:, None] + HALF * (np.arange(LANES)[None, :] >= HALF)
    angles = 2 * np.pi * angles / extent
    spin = jnp.asarray(np.stack([np.cos(angles), -np.sin(angles)]), jnp.float32)
    slots = lax.iota(jnp.int32, HALF)
    zero = (fam == 0).astype(jnp.int32)
    total = None
    for chunk, piece in enumerate(pieces):
        got = lax.all_to_all(
            piece, ("rows", "rep"), split_axis=0, concat_axis=0, tiled=True,
            axis_index_groups=groups,
        ).reshape(slabs, 2, -1, count // 2, LANES)
        subs = got.shape[2]
        first_col = OUTER * slots if chunk == 0 else OUTER // 2 + OUTER * (HALF - 1 - slots)
        col = jnp.where(fam == 0, first_col, fam + OUTER * (slots + HALF * chunk))
        fx = jnp.broadcast_to(signed_float(col, extent).reshape(subs, SUB, 1), (subs, SUB, LANES))
        with_edge = chunk == 0
        if with_edge:
            info = jnp.stack([HALF - 1 + zero, jnp.int32(1), zero])
        else:
            info = jnp.stack([jnp.int32(HALF - 1), 1 - zero, jnp.int32(0)])
        bin_block = (half_slabs, 1, OUTER, width, LANES)
        edge_shape = (subs, OUTER, 2, 2 * LANES)
        sums_shape = (subs, 3 * GROUPS, LOWS)
        out = pl.pallas_call(
            functools.partial(band_kernel, extent, with_edge),
            grid=(subs,),
            in_specs=[
                pl.BlockSpec(memory_space=pltpu.SMEM),
                pl.BlockSpec((slabs, 2, 1, count // 2, LANES), lambda i: (0, 0, i, 0, 0)),
                pl.BlockSpec(bin_block, lambda i, at=chunk: (at, 0, 0, 0, 0)),
                pl.BlockSpec(bin_block, lambda i, at=1 - chunk: (at, 1, 0, 0, 0)),
                pl.BlockSpec(spin.shape, lambda i: (0, 0, 0)),
                pl.BlockSpec(col_high.shape, lambda i: (0, 0)),
                pl.BlockSpec(col_low.shape, lambda i: (0, 0)),
                pl.BlockSpec((1, SUB, LANES), lambda i: (i, 0, 0)),
            ],
            out_specs=[pl.BlockSpec((1, 3 * GROUPS, LOWS), lambda i: (i, 0, 0))]
            + [pl.BlockSpec(edge_shape, lambda i: (0, 0, 0, 0))] * with_edge,
            out_shape=[jax.ShapeDtypeStruct(sums_shape, jnp.float32)]
            + [jax.ShapeDtypeStruct(edge_shape, jnp.float32)] * with_edge,
            scratch_shapes=[
                pltpu.VMEM((OUTER, LANES, LANES), jnp.float32),
                pltpu.VMEM((2, 2, 3, SUB, LANES), jnp.float32),
                pltpu.VMEM((2, 2, 2, SUB + width, LANES), jnp.float32),
            ],
            compiler_params=pltpu.CompilerParams(vmem_limit_bytes=48 * 2**20),
            name="band_sums",
        )(info, got, got_bins, got_bins, spin, col_high, col_low, fx)
        sums = out[0].sum(0)
        total = sums if total is None else total + sums
        if with_edge:
            special = edge_sums(
                out[1][0], got_bins[0, 0, :, 0], got_bins[half_slabs, 1, :, 0], extent
            )
            special = jnp.where(fam == 0, special, 0.0)
    partial_sums = total.reshape(3, NBINS) + special
    auto = NBINS / (extent * extent)
    cross = math.sqrt(auto)
    factors = jnp.array([auto, auto, cross], jnp.float32)[:, None]
    own = summed(partial_sums, "rows")
    own = (own + partner(own, "rep", 0)) * factors
    skies = [own]
    distance = 1
    while 1 << distance < reps:
        skies = skies + [partner(sky, "rep", distance) for sky in skies]
        distance += 1
    stacked = jnp.stack(skies)
    order = lax.iota(jnp.int32, len(skies)) ^ (member // 2)
    return jnp.take(stacked, order, axis=0) if len(skies) > 2 else jnp.where(
        member // 2 == 0, stacked, stacked[::-1]
    )


def solution(mesh):
    in_specs = (P("rep", "rows", None), P("rows", None), P(None, "rows"))
    out_specs = P()

    def on_any(maps, mask, bins):
        extent = bins.shape[0]
        families = 2 * lax.axis_size("rows")
        if extent == OUTER * LANES and families == OUTER // 2 and NBINS == GROUPS * LOWS:
            return on_device_fast(maps, mask, bins)
        return on_device(maps, mask, bins)

    return jax.shard_map(
        on_any, mesh=mesh, in_specs=in_specs, out_specs=out_specs, check_vma=False
    )
```

```python
import functools
import math

import jax
import jax.numpy as jnp
import numpy as np
from jax import lax
from jax.experimental import pallas as pl
from jax.experimental.pallas import tpu as pltpu
from jax.sharding import PartitionSpec as P


NBINS = 1024


precise = lax.Precision.HIGHEST


def partner(array, axis, distance):
    return lax.ppermute(array, axis, [(i, i ^ 1 << distance) for i in range(lax.axis_size(axis))])


def dft_table(count_a, count_b, period):
    first = lax.iota(jnp.int32, count_a)[:, None]
    second = lax.iota(jnp.int32, count_b)[None, :]
    angles = (first * second % period).astype(jnp.float32) * (2.0 * math.pi / period)
    return (jnp.cos(angles), -jnp.sin(angles))


def split_length(length):
    outer_len = 2 ** ((length.bit_length() - 1) // 2)
    return (outer_len, length // outer_len)


def complex_apply(form, real_part, imag_part, table_cos, table_sin):

    def product(left, right):
        return jnp.einsum(form, left, right, precision=precise)

    return (
        product(real_part, table_cos) - product(imag_part, table_sin),
        product(real_part, table_sin) + product(imag_part, table_cos),
    )


def twiddled(real_part, imag_part, table_cos, table_sin):
    return (
        real_part * table_cos - imag_part * table_sin,
        real_part * table_sin + imag_part * table_cos,
    )


def row_transform(values):
    count, length = values.shape
    outer_len, inner_len = split_length(length)
    outer_cos, outer_sin = dft_table(outer_len, outer_len, outer_len)
    inner_cos, inner_sin = dft_table(inner_len, inner_len, inner_len)
    turn_cos, turn_sin = dft_table(outer_len, inner_len, length)
    shaped = values.reshape(count, outer_len, inner_len)
    first_real = jnp.einsum("yan,ak->ykn", shaped, outer_cos, precision=precise)
    first_imag = jnp.einsum("yan,ak->ykn", shaped, outer_sin, precision=precise)
    mid_real, mid_imag = twiddled(first_real, first_imag, turn_cos, turn_sin)
    last_real, last_imag = complex_apply("ykn,nm->ymk", mid_real, mid_imag, inner_cos, inner_sin)
    return (last_real.reshape(count, length), last_imag.reshape(count, length))


def column_transform(pieces):
    real_part, imag_part = pieces
    length, groups, width = real_part.shape
    outer_len, inner_len = split_length(length)
    outer_cos, outer_sin = dft_table(outer_len, outer_len, outer_len)
    inner_cos, inner_sin = dft_table(inner_len, inner_len, inner_len)
    turn_cos, turn_sin = dft_table(outer_len, inner_len, length)
    shaped_real = real_part.reshape(outer_len, inner_len, groups, width)
    shaped_imag = imag_part.reshape(outer_len, inner_len, groups, width)
    first_real, first_imag = complex_apply(
        "anbc,ak->knbc", shaped_real, shaped_imag, outer_cos, outer_sin
    )
    mid_real, mid_imag = twiddled(
        first_real, first_imag, turn_cos[:, :, None, None], turn_sin[:, :, None, None]
    )
    last_real, last_imag = complex_apply("knbc,nm->mkbc", mid_real, mid_imag, inner_cos, inner_sin)
    return (last_real.reshape(length, groups, width), last_imag.reshape(length, groups, width))


def signed_float(indices, extent):
    return jnp.where(indices >= extent // 2, indices - extent, indices).astype(jnp.float32)


def band_terms(fields, freq_y, freq_x, bin_block, nbins_count, extent):
    q_real, q_imag, u_real, u_imag = fields
    radius = jnp.maximum(freq_x * freq_x + freq_y * freq_y, 1.0)
    cos_twice = (freq_x * freq_x - freq_y * freq_y) / radius
    sin_twice = 2.0 * freq_x * freq_y / radius
    e_real = cos_twice * q_real + sin_twice * u_real
    e_imag = cos_twice * q_imag + sin_twice * u_imag
    b_real = -sin_twice * q_real + cos_twice * u_real
    b_imag = -sin_twice * q_imag + cos_twice * u_imag
    inv_area = 1.0 / (extent * extent)
    powers = jnp.stack(
        [
            (e_real * e_real + e_imag * e_imag) * inv_area,
            (b_real * b_real + b_imag * b_imag) * inv_area,
            (e_real * b_real + e_imag * b_imag) * inv_area,
        ]
    ).astype(jnp.bfloat16)
    bit_count = nbins_count.bit_length() - 1
    high_count = 2 ** max(bit_count // 2 - 1, 0)
    low_count = nbins_count // high_count
    high_part = bin_block // low_count
    low_part = bin_block % low_count
    high_hot = (high_part[None] == lax.iota(jnp.int32, high_count)[:, None, None]).astype(
        jnp.bfloat16
    )
    weighted = (powers[:, None] * high_hot[None]).reshape(3 * high_count, -1)
    low_hot = (low_part[None] == lax.iota(jnp.int32, low_count)[:, None, None]).astype(jnp.bfloat16)
    low_hot = low_hot.reshape(low_count, -1)
    sums = lax.dot_general(
        weighted, low_hot, (((1,), (1,)), ((), ())), preferred_element_type=jnp.float32
    )
    return sums.reshape(3, nbins_count)


def on_device(maps, mask, bins):
    extent = bins.shape[0]
    columns = bins.shape[1]
    count = maps.shape[1]
    slab_index = lax.axis_index("rows")
    member = lax.axis_index("rep")
    pair_bit = member % 2
    field = maps[0] * mask.astype(jnp.float32)
    row_real, row_imag = row_transform(field)
    half_rows = extent // 2
    slabs = (
        row_real.reshape(count, extent // columns, columns),
        row_imag.reshape(count, extent // columns, columns),
    )
    spec_real, spec_imag = column_transform(
        (
            lax.all_to_all(slabs[0], "rows", split_axis=1, concat_axis=0, tiled=True),
            lax.all_to_all(slabs[1], "rows", split_axis=1, concat_axis=0, tiled=True),
        )
    )
    spec_real = spec_real.reshape(extent, columns)
    spec_imag = spec_imag.reshape(extent, columns)
    kept_real = lax.dynamic_slice_in_dim(spec_real, pair_bit * half_rows, half_rows, 0)
    kept_imag = lax.dynamic_slice_in_dim(spec_imag, pair_bit * half_rows, half_rows, 0)
    sent_real = lax.dynamic_slice_in_dim(spec_real, (1 - pair_bit) * half_rows, half_rows, 0)
    sent_imag = lax.dynamic_slice_in_dim(spec_imag, (1 - pair_bit) * half_rows, half_rows, 0)
    got_real, got_imag = partner((sent_real, sent_imag), "rep", 0)
    is_first = pair_bit == 0
    fields = (
        jnp.where(is_first, kept_real, got_real),
        jnp.where(is_first, kept_imag, got_imag),
        jnp.where(is_first, got_real, kept_real),
        jnp.where(is_first, got_imag, kept_imag),
    )
    own_bins = lax.dynamic_slice_in_dim(bins, pair_bit * half_rows, half_rows, 0)

    def frequency_of(offset, height):
        rows_here = lax.iota(jnp.int32, height)[:, None] + offset + pair_bit * half_rows
        cols_here = lax.iota(jnp.int32, columns)[None, :] + slab_index * columns
        return (rows_here, cols_here)

    block = min(256, half_rows)
    blocks = half_rows // block
    stacked = tuple((part.reshape(blocks, block, columns) for part in fields))
    bin_blocks = own_bins.reshape(blocks, block, columns)

    def accumulate(running, items):
        block_index, parts, bin_block = items
        rows_here, cols_here = frequency_of(block_index * block, block)
        term = band_terms(
            parts,
            signed_float(rows_here, extent),
            signed_float(cols_here, extent),
            bin_block,
            NBINS,
            extent,
        )
        return (running + term, None)

    partial_sums, _ = lax.scan(
        accumulate,
        jnp.zeros((3, NBINS), jnp.float32),
        (lax.iota(jnp.int32, blocks), stacked, bin_blocks),
    )
    sims_count = lax.axis_size("rep") // 2
    slot = (lax.iota(jnp.int32, sims_count) == member // 2).astype(jnp.float32)[:, None, None]
    totals = lax.psum(slot * partial_sums[None], ("rows", "rep"))
    auto = NBINS / (extent * extent)
    cross = math.sqrt(auto)
    factors = jnp.array([auto, auto, cross], jnp.float32)[None, :, None]
    return totals * factors


LANES = 128
OUTER = 32
HALF = LANES // 2
SUB = LANES // 4
GROUPS = 16
LOWS = 64


def fft_wave(index, size):
    return (math.cos(2 * math.pi * index / size), -math.sin(2 * math.pi * index / size))


def turned(value, index, size):
    real, imag = value
    if index == 0:
        return value
    if 4 * index == size:
        return (imag, -real)
    cosine, sine = fft_wave(index, size)
    if 8 * index == size:
        return ((real + imag) * cosine, (imag - real) * cosine)
    if 8 * index == 3 * size:
        return ((imag - real) * -cosine, (real + imag) * cosine)
    return (real * cosine - imag * sine, real * sine + imag * cosine)


def real_fft(values):
    size = len(values)
    if size == 2:
        return [(values[0] + values[1], None), (values[0] - values[1], None)]
    even = real_fft(values[0::2])
    odd = real_fft(values[1::2])
    half = size // 2
    out = [None] * (half + 1)
    out[0] = (even[0][0] + odd[0][0], None)
    out[half] = (even[0][0] - odd[0][0], None)
    quarter = size // 4
    out[quarter] = (even[quarter][0], -odd[quarter][0])
    for k in range(1, quarter):
        real, imag = turned(odd[k], k, size)
        out[k] = (even[k][0] + real, even[k][1] + imag)
        out[half - k] = (even[k][0] - real, imag - even[k][1])
    return out


def complex_fft(values):
    size = len(values)
    if size == 1:
        return values
    even = complex_fft(values[0::2])
    odd = complex_fft(values[1::2])
    half = size // 2
    out = [None] * size
    for k in range(half):
        real, imag = turned(odd[k], k, size)
        out[k] = (even[k][0] + real, even[k][1] + imag)
        out[k + half] = (even[k][0] - real, even[k][1] - imag)
    return out


def wave_matrix(angles):
    cosine, sine = np.cos(angles), np.sin(angles)
    return cosine, sine


def host_tables(extent):
    b = np.arange(LANES)[:, None]
    k = np.arange(LANES)[None, :]
    cosine, sine = wave_matrix(2 * np.pi * (b * k % LANES) / LANES)
    natural = np.concatenate(
        [np.concatenate([cosine, -sine], 1), np.concatenate([sine, cosine], 1)], 0
    )
    first = np.zeros((2 * LANES, 2 * LANES))
    first[:LANES, :HALF] = cosine[:, :HALF]
    first[:LANES, LANES : LANES + HALF] = -sine[:, :HALF]
    first[:LANES, LANES] = 1.0 - 2.0 * (np.arange(LANES) % 2)
    freq = OUTER // 2 + OUTER * (HALF - 1 - np.arange(HALF)[None, :])
    cosine, sine = wave_matrix(2 * np.pi * (b * freq % extent) / extent)
    first[LANES:, HALF:LANES] = cosine
    first[LANES:, LANES + HALF :] = -sine
    order = np.concatenate(
        [part + SUB * s + np.arange(SUB) for s in range(LANES // SUB) for part in (0, LANES)]
    )
    rows = np.concatenate([part + HALF * h + np.arange(HALF) for h in range(2) for part in (0, LANES)])
    return first[:, order], natural[:, order], natural[rows]


def split_table(table):
    table = jnp.asarray(table, jnp.float32)
    high = table.astype(jnp.bfloat16)
    return high, (table - high.astype(jnp.float32)).astype(jnp.bfloat16)


def split_value(value):
    high = value.astype(jnp.bfloat16)
    return high, (value - high.astype(jnp.float32)).astype(jnp.bfloat16)


def dot_f32(left, right, dims=(((1,), (0,)), ((), ()))):
    return lax.dot_general(left, right, dims, preferred_element_type=jnp.float32)


def three_pass(value, table_high, table_low):
    high, low = split_value(value)
    return dot_f32(high, table_high) + (dot_f32(low, table_high) + dot_f32(high, table_low))


def row_kernel(
    map_ref, mask_ref, turn_ref, high_ref, low_ref, *refs
):
    out_refs, mid_ref = refs[:-1], refs[-1]
    block = map_ref.shape[1]
    left = lax.broadcasted_iota(jnp.int32, (block // 2, LANES), 1) < HALF

    def tile(step, carry):
        start = pl.multiple_of(step * 8, 8)
        cells = []
        for a in range(OUTER):
            lanes = pl.ds(a * LANES, LANES)
            weight = mask_ref[pl.ds(start, 8), lanes].astype(jnp.float32)
            cells.append(map_ref[0, pl.ds(start, 8), lanes] * weight)
        waves = real_fft(cells)
        half = OUTER // 2
        mid_ref[0, pl.ds(start, 8), 0:LANES] = waves[0][0]
        mid_ref[0, pl.ds(start, 8), LANES : 2 * LANES] = waves[half][0]
        for k in range(1, half):
            real, imag = waves[k]
            cosine = turn_ref[0, k : k + 1, :]
            sine = turn_ref[1, k : k + 1, :]
            mid_ref[k, pl.ds(start, 8), 0:LANES] = real * cosine - imag * sine
            mid_ref[k, pl.ds(start, 8), LANES : 2 * LANES] = real * sine + imag * cosine
        return carry

    lax.fori_loop(0, block // 8, tile, 0)

    def family(k, carry):
        which = jnp.minimum(k, 1)
        value = three_pass(mid_ref[k], high_ref[which], low_ref[which])
        subs = []
        for lanes in (slice(0, LANES), slice(LANES, 2 * LANES)):
            top, low = value[: block // 2, lanes], value[block // 2 :, lanes]
            subs.append(jnp.where(left, top, pltpu.roll(low, HALF, 1)))
            subs.append(jnp.where(left, pltpu.roll(top, HALF, 1), low))
        for out_ref, value in zip(out_refs, subs):
            out_ref[k] = value
        return carry

    lax.fori_loop(0, OUTER // 2, family, 0)


def bins_kernel(info_ref, flip_ref, *refs):
    bins_refs, out_ref, turn_ref = refs[:-2], refs[-2], refs[-1]
    step = pl.program_id(0)
    sub = bins_refs[0].shape[1]
    parity = info_ref[0]
    upper = info_ref[1]
    dests = out_ref.shape[0]
    width = out_ref.shape[3]
    zero = parity == 0
    high_side = upper == 1
    flat_refs = [ref.reshape(LANES * sub, LANES) for ref in bins_refs]
    for c in range(sub):
        kappa = step * sub + c
        mirrored = (OUTER - kappa) % OUTER
        for part, ref in enumerate(flat_refs):
            turn_ref[c % 2, part * LANES : (part + 1) * LANES] = (
                ref[pl.ds(c, LANES, stride=sub), :].astype(jnp.float32).T
            )

        def column(at):
            return turn_ref[c % 2, pl.ds(at, width, stride=OUTER), :]

        ahead = [column(jnp.where(zero & high_side, OUTER // 2, parity))]
        back = [column(jnp.where(zero, jnp.where(high_side, 0, OUTER // 2), OUTER - parity))]
        for dest in range(1, dests):
            ahead.append(column(2 * dest + parity))
            back.append(column(OUTER - 2 * dest - parity))
        mixed = jnp.concatenate([ahead[0]] + back, 0)
        high = jnp.floor(mixed * 0.125)
        pair = jnp.concatenate([high.astype(jnp.bfloat16), (mixed - high * 8.0).astype(jnp.bfloat16)], 1)
        flipped = dot_f32(pair, flip_ref[jnp.minimum(kappa, 1)])
        turn0 = zero & high_side
        turn1 = jnp.logical_not(zero & jnp.logical_not(high_side))
        out_ref[0, 0, jnp.where(turn0, mirrored, kappa)] = jnp.where(turn0, flipped[:width], ahead[0])
        out_ref[0, 1, jnp.where(turn1, mirrored, kappa)] = jnp.where(
            turn1, flipped[width : 2 * width], back[0]
        )
        for dest in range(1, dests):
            out_ref[dest, 0, kappa] = ahead[dest]
            out_ref[dest, 1, mirrored] = flipped[(dest + 1) * width : (dest + 2) * width]


def band_kernel(
    extent, half_chunk, with_edge, info_ref, x_ref, bins0_ref, bins1_ref, turn_ref, high_ref, low_ref,
    fx_ref, *refs,
):
    if with_edge:
        sums_ref, edge_ref, mid_ref, power_ref, part_ref = refs
    else:
        sums_ref, mid_ref, power_ref, part_ref = refs
    sub = half_chunk
    offset = info_ref[0]
    flipped = info_ref[1]
    hollow = (info_ref[2] == 1) if sub == 0 else False
    per_slab = x_ref.shape[3] // HALF
    even8 = lax.broadcasted_iota(jnp.int32, (8, LANES), 1) % HALF < SUB

    def tile(step, carry):
        start = pl.multiple_of(step * 8, 8)
        cells = []
        for a in range(OUTER):
            rows = pl.ds((a % per_slab) * HALF + start, 8)
            q = x_ref[a // per_slab, 0, 0, rows, :]
            u = x_ref[a // per_slab, 1, 0, rows, :]
            real = jnp.where(even8, q, pltpu.roll(u, SUB, 1))
            imag = jnp.where(even8, pltpu.roll(q, LANES - SUB, 1), u)
            cells.append((real, imag))
        waves = complex_fft(cells)
        turns = {1: (turn_ref[0, pl.ds(start, 8), :], turn_ref[1, pl.ds(start, 8), :])}
        mid_ref[0, pl.ds(start, 8), :] = waves[0][0]
        mid_ref[0, pl.ds(HALF + start, 8), :] = waves[0][1]
        for k in range(1, OUTER):
            if k not in turns:
                (ar, ai), (br, bi) = turns[k // 2], turns[k - k // 2]
                turns[k] = (ar * br - ai * bi, ar * bi + ai * br)
            cosine, sine = turns[k]
            real, imag = waves[k]
            mid_ref[k, pl.ds(start, 8), :] = real * cosine - imag * sine
            mid_ref[k, pl.ds(HALF + start, 8), :] = real * sine + imag * cosine
        return carry

    lax.fori_loop(0, HALF // 8, tile, 0)

    fx = fx_ref[0]
    lane = lax.broadcasted_iota(jnp.int32, (SUB, LANES), 1)
    slot = lax.broadcasted_iota(jnp.int32, (SUB, LANES), 0)
    keep = jnp.where((slot == 0) & hollow, 0.0, 1.0) if sub == 0 else 1.0
    inv_area = 1.0 / (extent * extent)
    group_iota = lax.broadcasted_iota(jnp.int32, (GROUPS, LANES), 0).astype(jnp.float32).astype(jnp.bfloat16)
    low_iota = lax.broadcasted_iota(jnp.int32, (LOWS, LANES), 0).astype(jnp.float32).astype(jnp.bfloat16)
    width = bins0_ref.shape[3]
    near = SUB // width
    one = jnp.ones((LOWS, LANES), jnp.bfloat16)
    none = jnp.zeros((LOWS, LANES), jnp.bfloat16)
    empty = jnp.zeros((GROUPS, LANES), jnp.bfloat16)
    begin0 = sub * near
    begin1 = (1 - sub) * near

    def pair(step, acc):
        turned_rows = []
        for member in range(2):
            flat = mid_ref[2 * step + member].T
            turned_rows.append(jnp.concatenate([flat[:HALF], flat[HALF:]], 1))
        spectra = three_pass(jnp.concatenate(turned_rows, 0), high_ref[...], low_ref[...])
        weighted, lows = [], []
        for member in range(2):
            k = 2 * step + member
            spectrum = spectra[member * HALF : (member + 1) * HALF]
            if with_edge:
                edge_ref[sub, k, 0:1, :] = spectrum[0:1, :]
                edge_ref[sub, k, 1:2, :] = spectrum[SUB : SUB + 1, :]
            q_real, q_imag = spectrum[:SUB, :LANES], spectrum[:SUB, LANES:]
            u_real, u_imag = spectrum[SUB:, :LANES], spectrum[SUB:, LANES:]
            row = lane * OUTER + k
            fy = jnp.where(row >= extent // 2, row - extent, row).astype(jnp.float32)
            radius = jnp.maximum(fx * fx + fy * fy, 1.0)
            cos_twice = (fx * fx - fy * fy) / radius
            sin_twice = 2.0 * fx * fy / radius

            def powers(sine, which):
                e_real = cos_twice * q_real + sine * u_real
                e_imag = cos_twice * q_imag + sine * u_imag
                b_real = cos_twice * u_real - sine * q_real
                b_imag = cos_twice * u_imag - sine * q_imag
                power_ref[member, which, 0] = (e_real * e_real + e_imag * e_imag) * inv_area * keep
                power_ref[member, which, 1] = (b_real * b_real + b_imag * b_imag) * inv_area * keep
                power_ref[member, which, 2] = (e_real * b_real + e_imag * b_imag) * inv_area * keep

            other = 0
            if member == 0:
                other = jnp.where(k == 0, 1, 0)
                powers(sin_twice, jnp.where(k == 0, 1 - flipped, 0))

                @pl.when(k == 0)
                def _():
                    powers(jnp.where(row == extent // 2, -sin_twice, sin_twice), flipped)

            else:
                powers(sin_twice, 0)

            for index, (bins_ref, begin, count) in enumerate(
                ((bins0_ref, begin0, near), (bins1_ref, begin1, near + 1))
            ):
                for source in range(count):
                    at = min(begin + source, bins_ref.shape[0] - 1)
                    value = bins_ref[at, 0, k]
                    high = jnp.floor(value * (1.0 / LOWS))
                    rows = slice(source * width, (source + 1) * width)
                    part_ref[member, index, 0, rows] = high
                    part_ref[member, index, 1, rows] = value - high * LOWS

            for i in range(SUB):
                mirror = offset - HALF + SUB - i
                for index, at, source in ((0, i, 0), (1, mirror, other)):
                    high = part_ref[member, index, 0, pl.ds(at, 1), :]
                    low = part_ref[member, index, 1, pl.ds(at, 1), :]
                    high = jnp.broadcast_to(high, (GROUPS, LANES)).astype(jnp.bfloat16)
                    low = jnp.broadcast_to(low, (LOWS, LANES)).astype(jnp.bfloat16)
                    hot = high == group_iota
                    column = []
                    for kind in range(3):
                        power = power_ref[member, source, kind, pl.ds(i, 1), :]
                        power = jnp.broadcast_to(power, (GROUPS, LANES)).astype(jnp.bfloat16)
                        column.append(jnp.where(hot, power, empty))
                    weighted.append(jnp.concatenate(column, 0))
                    lows.append(jnp.where(low == low_iota, one, none))
        return acc + dot_f32(
            jnp.concatenate(weighted, 1), jnp.concatenate(lows, 1), (((1,), (1,)), ((), ()))
        )

    sums_ref[0] = lax.fori_loop(0, OUTER // 2, pair, jnp.zeros((3 * GROUPS, LOWS), jnp.float32))


def summed(array, axis):
    distance = 0
    while 1 << distance < lax.axis_size(axis):
        array = array + partner(array, axis, distance)
        distance += 1
    return array


def edge_sums(edge, bins_left, bins_right, extent):
    flat = edge.transpose(1, 2, 0).reshape(2, 2, extent)
    back = jnp.roll(flat[:, :, ::-1], 1, axis=2)
    q_real, q_imag, u_real, u_imag = [
        jnp.stack(pair)
        for m in range(2)
        for pair in (
            (0.5 * (flat[m, 0] + back[m, 0]), 0.5 * (flat[m, 1] + back[m, 1])),
            (0.5 * (flat[m, 1] - back[m, 1]), 0.5 * (back[m, 0] - flat[m, 0])),
        )
    ]
    freq_y = signed_float(lax.iota(jnp.int32, extent), extent)[None, :]
    freq_x = jnp.array([0.0, -extent // 2], jnp.float32)[:, None]
    left = bins_left.T.reshape(extent)
    right = jnp.roll(bins_right.T.reshape(extent)[::-1], 1)
    bins = jnp.stack([left, right]).astype(jnp.int32)
    return band_terms((q_real, q_imag, u_real, u_imag), freq_y, freq_x, bins, NBINS, extent)


def on_device_fast(maps, mask, bins):
    extent = bins.shape[0]
    columns = bins.shape[1]
    count = maps.shape[1]
    slabs = lax.axis_size("rows")
    reps = lax.axis_size("rep")
    slab_index = lax.axis_index("rows")
    member = lax.axis_index("rep")
    pair_bit = member % 2
    half_slabs = slabs // 2
    first, family, natural = host_tables(extent)
    row_high, row_low = split_table(np.stack([first, family]))
    col_high, col_low = split_table(natural)

    flips = np.zeros((2, 2 * LANES, LANES))
    for k in range(LANES):
        flips[0, k, -k % LANES] = 8.0
        flips[0, LANES + k, -k % LANES] = 1.0
        flips[1, k, LANES - 1 - k] = 8.0
        flips[1, LANES + k, LANES - 1 - k] = 1.0
    info = jnp.stack([pair_bit, (slab_index >= half_slabs).astype(jnp.int32)])
    sub = 8
    width = columns // OUTER
    sent_bins = pl.pallas_call(
        bins_kernel,
        grid=(OUTER // sub,),
        in_specs=[
            pl.BlockSpec(memory_space=pltpu.SMEM),
            pl.BlockSpec((2, 2 * LANES, LANES), lambda i: (0, 0, 0)),
        ]
        + [
            pl.BlockSpec((LANES, sub, LANES), lambda i, part=part: (0, i, part))
            for part in range(columns // LANES)
        ],
        out_specs=pl.BlockSpec((slabs, 2, OUTER, width, LANES), lambda i: (0, 0, 0, 0, 0)),
        out_shape=jax.ShapeDtypeStruct((slabs, 2, OUTER, width, LANES), jnp.float32),
        scratch_shapes=[pltpu.VMEM((2, columns, LANES), jnp.float32)],
        cost_estimate=pl.CostEstimate(flops=5 * 10**9, transcendentals=0, bytes_accessed=12 * 2**20),
        name="bins_prep",
    )(info, jnp.asarray(flips, jnp.bfloat16), *[bins.reshape(LANES, OUTER, columns)] * (columns // LANES))
    got_bins = lax.all_to_all(sent_bins, "rows", split_axis=0, concat_axis=0, tiled=True)

    block = min(LANES, count)
    k1 = np.arange(OUTER // 2)[:, None]
    angles = 2 * np.pi * (k1 * np.arange(LANES)[None, :] % extent) / extent
    turns = jnp.asarray(np.stack([np.cos(angles), -np.sin(angles)]), jnp.float32)
    table_spec = pl.BlockSpec((2, 2 * LANES, 2 * LANES), lambda i: (0, 0, 0))
    piece = jax.ShapeDtypeStruct((2 * slabs, count // 2, LANES), jnp.float32)
    piece_spec = pl.BlockSpec((2 * slabs, block // 2, LANES), lambda i: (0, i, 0))
    pieces = pl.pallas_call(
        row_kernel,
        grid=(count // block,),
        in_specs=[
            pl.BlockSpec((1, block, extent), lambda i: (0, i, 0)),
            pl.BlockSpec((block, extent), lambda i: (i, 0)),
            pl.BlockSpec(turns.shape, lambda i: (0, 0, 0)),
            table_spec,
            table_spec,
        ],
        out_specs=[piece_spec] * (LANES // SUB),
        out_shape=[piece] * (LANES // SUB),
        scratch_shapes=[pltpu.VMEM((OUTER // 2, block, 2 * LANES), jnp.float32)],
        cost_estimate=pl.CostEstimate(flops=12 * 10**9, transcendentals=0, bytes_accessed=24 * 2**20),
        name="row_fft",
    )(maps, mask, turns, row_high, row_low)

    groups = [
        [row * reps + z for row in range(slabs) for z in (2 * sky, 2 * sky + 1)]
        for sky in range(reps // 2)
    ]
    fam = 2 * slab_index + pair_bit
    angles = np.arange(HALF)[:, None] + HALF * (np.arange(LANES)[None, :] >= HALF)
    angles = 2 * np.pi * angles / extent
    spin = jnp.asarray(np.stack([np.cos(angles), -np.sin(angles)]), jnp.float32)
    slots = lax.iota(jnp.int32, HALF)
    zero = (fam == 0).astype(jnp.int32)
    total = None
    before = got_bins
    for number, piece in enumerate(pieces):
        chunk, half_chunk = number // 2, number % 2
        piece, before = lax.optimization_barrier((piece, before))
        got = lax.all_to_all(
            piece, ("rows", "rep"), split_axis=0, concat_axis=0, tiled=True,
            axis_index_groups=groups,
        )
        before = got
        got = got.reshape(slabs, 2, -1, count // 2, LANES)
        subs = got.shape[2]
        first_col = OUTER * slots if chunk == 0 else OUTER // 2 + OUTER * (HALF - 1 - slots)
        col = jnp.where(fam == 0, first_col, fam + OUTER * (slots + HALF * chunk))
        col = col[half_chunk * SUB : (half_chunk + 1) * SUB]
        fx = jnp.broadcast_to(signed_float(col, extent).reshape(subs, SUB, 1), (subs, SUB, LANES))
        with_edge = number == 0
        if chunk == 0:
            info = jnp.stack([HALF - 1 + zero, jnp.int32(1), zero])
        else:
            info = jnp.stack([jnp.int32(HALF - 1), 1 - zero, jnp.int32(0)])
        if number == 1:
            info, special = lax.optimization_barrier((info, special))
        bin_block = (half_slabs, 1, OUTER, width, LANES)
        edge_shape = (subs, OUTER, 2, 2 * LANES)
        sums_shape = (subs, 3 * GROUPS, LOWS)
        band_call = pl.pallas_call(
            functools.partial(band_kernel, extent, half_chunk, with_edge),
            grid=(subs,),
            in_specs=[
                pl.BlockSpec(memory_space=pltpu.SMEM),
                pl.BlockSpec((slabs, 2, 1, count // 2, LANES), lambda i: (0, 0, i, 0, 0)),
                pl.BlockSpec(bin_block, lambda i, at=chunk: (at, 0, 0, 0, 0)),
                pl.BlockSpec(bin_block, lambda i, at=1 - chunk: (at, 1, 0, 0, 0)),
                pl.BlockSpec(spin.shape, lambda i: (0, 0, 0)),
                pl.BlockSpec(col_high.shape, lambda i: (0, 0)),
                pl.BlockSpec(col_low.shape, lambda i: (0, 0)),
                pl.BlockSpec((1, SUB, LANES), lambda i: (i, 0, 0)),
            ],
            out_specs=[pl.BlockSpec((1, 3 * GROUPS, LOWS), lambda i: (i, 0, 0))]
            + [pl.BlockSpec(edge_shape, lambda i: (0, 0, 0, 0))] * with_edge,
            out_shape=[jax.ShapeDtypeStruct(sums_shape, jnp.float32)]
            + [jax.ShapeDtypeStruct(edge_shape, jnp.float32)] * with_edge,
            scratch_shapes=[
                pltpu.VMEM((OUTER, LANES, LANES), jnp.float32),
                pltpu.VMEM((2, 2, 3, SUB, LANES), jnp.float32),
                pltpu.VMEM((2, 2, 2, SUB + width, LANES), jnp.float32),
            ],
            compiler_params=pltpu.CompilerParams(vmem_limit_bytes=48 * 2**20),
            cost_estimate=pl.CostEstimate(flops=10**10, transcendentals=0, bytes_accessed=4 * 2**20),
            name="band_sums",
        )
        out = band_call(info, got, got_bins, got_bins, spin, col_high, col_low, fx)
        sums = out[0].sum(0)
        total = sums if total is None else total + sums
        if with_edge:
            special = edge_sums(
                out[1][0], got_bins[0, 0, :, 0], got_bins[half_slabs, 1, :, 0], extent
            )
            special = jnp.where(fam == 0, special, 0.0)
    partial_sums = total.reshape(3, NBINS) + special
    auto = NBINS / (extent * extent)
    cross = math.sqrt(auto)
    factors = jnp.array([auto, auto, cross], jnp.float32)[:, None]
    own = summed(partial_sums, "rows")
    own = (own + partner(own, "rep", 0)) * factors
    skies = [own]
    distance = 1
    while 1 << distance < reps:
        skies = skies + [partner(sky, "rep", distance) for sky in skies]
        distance += 1
    stacked = jnp.stack(skies)
    order = lax.iota(jnp.int32, len(skies)) ^ (member // 2)
    return jnp.take(stacked, order, axis=0) if len(skies) > 2 else jnp.where(
        member // 2 == 0, stacked, stacked[::-1]
    )


def solution(mesh):
    in_specs = (P("rep", "rows", None), P("rows", None), P(None, "rows"))
    out_specs = P()

    def on_any(maps, mask, bins):
        extent = bins.shape[0]
        families = 2 * lax.axis_size("rows")
        if extent == OUTER * LANES and families == OUTER // 2 and NBINS == GROUPS * LOWS:
            return on_device_fast(maps, mask, bins)
        return on_device(maps, mask, bins)

    return jax.shard_map(
        on_any, mesh=mesh, in_specs=in_specs, out_specs=out_specs, check_vma=False
    )
```

```python
import functools
import math

import jax
import jax.numpy as jnp
import numpy as np
from jax import lax
from jax.experimental import pallas as pl
from jax.experimental.pallas import tpu as pltpu
from jax.sharding import PartitionSpec as P


NBINS = 1024


precise = lax.Precision.HIGHEST


def partner(array, axis, distance):
    return lax.ppermute(array, axis, [(i, i ^ 1 << distance) for i in range(lax.axis_size(axis))])


def dft_table(count_a, count_b, period):
    first = lax.iota(jnp.int32, count_a)[:, None]
    second = lax.iota(jnp.int32, count_b)[None, :]
    angles = (first * second % period).astype(jnp.float32) * (2.0 * math.pi / period)
    return (jnp.cos(angles), -jnp.sin(angles))


def split_length(length):
    outer_len = 2 ** ((length.bit_length() - 1) // 2)
    return (outer_len, length // outer_len)


def complex_apply(form, real_part, imag_part, table_cos, table_sin):

    def product(left, right):
        return jnp.einsum(form, left, right, precision=precise)

    return (
        product(real_part, table_cos) - product(imag_part, table_sin),
        product(real_part, table_sin) + product(imag_part, table_cos),
    )


def twiddled(real_part, imag_part, table_cos, table_sin):
    return (
        real_part * table_cos - imag_part * table_sin,
        real_part * table_sin + imag_part * table_cos,
    )


def row_transform(values):
    count, length = values.shape
    outer_len, inner_len = split_length(length)
    outer_cos, outer_sin = dft_table(outer_len, outer_len, outer_len)
    inner_cos, inner_sin = dft_table(inner_len, inner_len, inner_len)
    turn_cos, turn_sin = dft_table(outer_len, inner_len, length)
    shaped = values.reshape(count, outer_len, inner_len)
    first_real = jnp.einsum("yan,ak->ykn", shaped, outer_cos, precision=precise)
    first_imag = jnp.einsum("yan,ak->ykn", shaped, outer_sin, precision=precise)
    mid_real, mid_imag = twiddled(first_real, first_imag, turn_cos, turn_sin)
    last_real, last_imag = complex_apply("ykn,nm->ymk", mid_real, mid_imag, inner_cos, inner_sin)
    return (last_real.reshape(count, length), last_imag.reshape(count, length))


def column_transform(pieces):
    real_part, imag_part = pieces
    length, groups, width = real_part.shape
    outer_len, inner_len = split_length(length)
    outer_cos, outer_sin = dft_table(outer_len, outer_len, outer_len)
    inner_cos, inner_sin = dft_table(inner_len, inner_len, inner_len)
    turn_cos, turn_sin = dft_table(outer_len, inner_len, length)
    shaped_real = real_part.reshape(outer_len, inner_len, groups, width)
    shaped_imag = imag_part.reshape(outer_len, inner_len, groups, width)
    first_real, first_imag = complex_apply(
        "anbc,ak->knbc", shaped_real, shaped_imag, outer_cos, outer_sin
    )
    mid_real, mid_imag = twiddled(
        first_real, first_imag, turn_cos[:, :, None, None], turn_sin[:, :, None, None]
    )
    last_real, last_imag = complex_apply("knbc,nm->mkbc", mid_real, mid_imag, inner_cos, inner_sin)
    return (last_real.reshape(length, groups, width), last_imag.reshape(length, groups, width))


def signed_float(indices, extent):
    return jnp.where(indices >= extent // 2, indices - extent, indices).astype(jnp.float32)


def band_terms(fields, freq_y, freq_x, bin_block, nbins_count, extent):
    q_real, q_imag, u_real, u_imag = fields
    radius = jnp.maximum(freq_x * freq_x + freq_y * freq_y, 1.0)
    cos_twice = (freq_x * freq_x - freq_y * freq_y) / radius
    sin_twice = 2.0 * freq_x * freq_y / radius
    e_real = cos_twice * q_real + sin_twice * u_real
    e_imag = cos_twice * q_imag + sin_twice * u_imag
    b_real = -sin_twice * q_real + cos_twice * u_real
    b_imag = -sin_twice * q_imag + cos_twice * u_imag
    inv_area = 1.0 / (extent * extent)
    powers = jnp.stack(
        [
            (e_real * e_real + e_imag * e_imag) * inv_area,
            (b_real * b_real + b_imag * b_imag) * inv_area,
            (e_real * b_real + e_imag * b_imag) * inv_area,
        ]
    ).astype(jnp.bfloat16)
    bit_count = nbins_count.bit_length() - 1
    high_count = 2 ** max(bit_count // 2 - 1, 0)
    low_count = nbins_count // high_count
    high_part = bin_block // low_count
    low_part = bin_block % low_count
    high_hot = (high_part[None] == lax.iota(jnp.int32, high_count)[:, None, None]).astype(
        jnp.bfloat16
    )
    weighted = (powers[:, None] * high_hot[None]).reshape(3 * high_count, -1)
    low_hot = (low_part[None] == lax.iota(jnp.int32, low_count)[:, None, None]).astype(jnp.bfloat16)
    low_hot = low_hot.reshape(low_count, -1)
    sums = lax.dot_general(
        weighted, low_hot, (((1,), (1,)), ((), ())), preferred_element_type=jnp.float32
    )
    return sums.reshape(3, nbins_count)


def on_device(maps, mask, bins):
    extent = bins.shape[0]
    columns = bins.shape[1]
    count = maps.shape[1]
    slab_index = lax.axis_index("rows")
    member = lax.axis_index("rep")
    pair_bit = member % 2
    field = maps[0] * mask.astype(jnp.float32)
    row_real, row_imag = row_transform(field)
    half_rows = extent // 2
    slabs = (
        row_real.reshape(count, extent // columns, columns),
        row_imag.reshape(count, extent // columns, columns),
    )
    spec_real, spec_imag = column_transform(
        (
            lax.all_to_all(slabs[0], "rows", split_axis=1, concat_axis=0, tiled=True),
            lax.all_to_all(slabs[1], "rows", split_axis=1, concat_axis=0, tiled=True),
        )
    )
    spec_real = spec_real.reshape(extent, columns)
    spec_imag = spec_imag.reshape(extent, columns)
    kept_real = lax.dynamic_slice_in_dim(spec_real, pair_bit * half_rows, half_rows, 0)
    kept_imag = lax.dynamic_slice_in_dim(spec_imag, pair_bit * half_rows, half_rows, 0)
    sent_real = lax.dynamic_slice_in_dim(spec_real, (1 - pair_bit) * half_rows, half_rows, 0)
    sent_imag = lax.dynamic_slice_in_dim(spec_imag, (1 - pair_bit) * half_rows, half_rows, 0)
    got_real, got_imag = partner((sent_real, sent_imag), "rep", 0)
    is_first = pair_bit == 0
    fields = (
        jnp.where(is_first, kept_real, got_real),
        jnp.where(is_first, kept_imag, got_imag),
        jnp.where(is_first, got_real, kept_real),
        jnp.where(is_first, got_imag, kept_imag),
    )
    own_bins = lax.dynamic_slice_in_dim(bins, pair_bit * half_rows, half_rows, 0)

    def frequency_of(offset, height):
        rows_here = lax.iota(jnp.int32, height)[:, None] + offset + pair_bit * half_rows
        cols_here = lax.iota(jnp.int32, columns)[None, :] + slab_index * columns
        return (rows_here, cols_here)

    block = min(256, half_rows)
    blocks = half_rows // block
    stacked = tuple((part.reshape(blocks, block, columns) for part in fields))
    bin_blocks = own_bins.reshape(blocks, block, columns)

    def accumulate(running, items):
        block_index, parts, bin_block = items
        rows_here, cols_here = frequency_of(block_index * block, block)
        term = band_terms(
            parts,
            signed_float(rows_here, extent),
            signed_float(cols_here, extent),
            bin_block,
            NBINS,
            extent,
        )
        return (running + term, None)

    partial_sums, _ = lax.scan(
        accumulate,
        jnp.zeros((3, NBINS), jnp.float32),
        (lax.iota(jnp.int32, blocks), stacked, bin_blocks),
    )
    sims_count = lax.axis_size("rep") // 2
    slot = (lax.iota(jnp.int32, sims_count) == member // 2).astype(jnp.float32)[:, None, None]
    totals = lax.psum(slot * partial_sums[None], ("rows", "rep"))
    auto = NBINS / (extent * extent)
    cross = math.sqrt(auto)
    factors = jnp.array([auto, auto, cross], jnp.float32)[None, :, None]
    return totals * factors


LANES = 128
OUTER = 32
HALF = LANES // 2
SUB = LANES // 4
BATCH = 4
GROUPS = 16
LOWS = 64


def fft_wave(index, size):
    return (math.cos(2 * math.pi * index / size), -math.sin(2 * math.pi * index / size))


def turned(value, index, size):
    real, imag = value
    if index == 0:
        return value
    if 4 * index == size:
        return (imag, -real)
    cosine, sine = fft_wave(index, size)
    if 8 * index == size:
        return ((real + imag) * cosine, (imag - real) * cosine)
    if 8 * index == 3 * size:
        return ((imag - real) * -cosine, (real + imag) * cosine)
    return (real * cosine - imag * sine, real * sine + imag * cosine)


def real_fft(values):
    size = len(values)
    if size == 2:
        return [(values[0] + values[1], None), (values[0] - values[1], None)]
    even = real_fft(values[0::2])
    odd = real_fft(values[1::2])
    half = size // 2
    out = [None] * (half + 1)
    out[0] = (even[0][0] + odd[0][0], None)
    out[half] = (even[0][0] - odd[0][0], None)
    quarter = size // 4
    out[quarter] = (even[quarter][0], -odd[quarter][0])
    for k in range(1, quarter):
        real, imag = turned(odd[k], k, size)
        out[k] = (even[k][0] + real, even[k][1] + imag)
        out[half - k] = (even[k][0] - real, imag - even[k][1])
    return out


def complex_fft(values):
    size = len(values)
    if size == 1:
        return values
    even = complex_fft(values[0::2])
    odd = complex_fft(values[1::2])
    half = size // 2
    out = [None] * size
    for k in range(half):
        real, imag = turned(odd[k], k, size)
        out[k] = (even[k][0] + real, even[k][1] + imag)
        out[k + half] = (even[k][0] - real, even[k][1] - imag)
    return out


def wave_matrix(angles):
    cosine, sine = np.cos(angles), np.sin(angles)
    return cosine, sine


def host_tables(extent):
    b = np.arange(LANES)[:, None]
    k = np.arange(LANES)[None, :]
    cosine, sine = wave_matrix(2 * np.pi * (b * k % LANES) / LANES)
    natural = np.concatenate(
        [np.concatenate([cosine, -sine], 1), np.concatenate([sine, cosine], 1)], 0
    )
    first = np.zeros((2 * LANES, 2 * LANES))
    first[:LANES, :HALF] = cosine[:, :HALF]
    first[:LANES, LANES : LANES + HALF] = -sine[:, :HALF]
    first[:LANES, LANES] = 1.0 - 2.0 * (np.arange(LANES) % 2)
    freq = OUTER // 2 + OUTER * (HALF - 1 - np.arange(HALF)[None, :])
    cosine, sine = wave_matrix(2 * np.pi * (b * freq % extent) / extent)
    first[LANES:, HALF:LANES] = cosine
    first[LANES:, LANES + HALF :] = -sine
    order = np.concatenate(
        [part + SUB * s + np.arange(SUB) for s in range(LANES // SUB) for part in (0, LANES)]
    )
    rows = np.concatenate([part + HALF * h + np.arange(HALF) for h in range(2) for part in (0, LANES)])
    return first[:, order], natural[:, order], natural[rows]


def split_table(table):
    table = jnp.asarray(table, jnp.float32)
    high = table.astype(jnp.bfloat16)
    return high, (table - high.astype(jnp.float32)).astype(jnp.bfloat16)


def split_value(value):
    high = value.astype(jnp.bfloat16)
    return high, (value - high.astype(jnp.float32)).astype(jnp.bfloat16)


def dot_f32(left, right, dims=(((1,), (0,)), ((), ()))):
    return lax.dot_general(left, right, dims, preferred_element_type=jnp.float32)


def three_pass(value, table_high, table_low):
    high, low = split_value(value)
    return dot_f32(high, table_high) + (dot_f32(low, table_high) + dot_f32(high, table_low))


def row_kernel(
    map_ref, mask_ref, turn_ref, high_ref, low_ref, *refs
):
    out_refs, mid_ref = refs[:-1], refs[-1]
    block = map_ref.shape[1]
    left = lax.broadcasted_iota(jnp.int32, (block // 2, LANES), 1) < HALF

    def tile(step, carry):
        start = pl.multiple_of(step * 8, 8)
        cells = []
        for a in range(OUTER):
            lanes = pl.ds(a * LANES, LANES)
            weight = mask_ref[pl.ds(start, 8), lanes].astype(jnp.float32)
            cells.append(map_ref[0, pl.ds(start, 8), lanes] * weight)
        waves = real_fft(cells)
        half = OUTER // 2
        mid_ref[0, pl.ds(start, 8), 0:LANES] = waves[0][0]
        mid_ref[0, pl.ds(start, 8), LANES : 2 * LANES] = waves[half][0]
        for k in range(1, half):
            real, imag = waves[k]
            cosine = turn_ref[0, k : k + 1, :]
            sine = turn_ref[1, k : k + 1, :]
            mid_ref[k, pl.ds(start, 8), 0:LANES] = real * cosine - imag * sine
            mid_ref[k, pl.ds(start, 8), LANES : 2 * LANES] = real * sine + imag * cosine
        return carry

    lax.fori_loop(0, block // 8, tile, 0)

    def family(k, carry):
        which = jnp.minimum(k, 1)
        value = three_pass(mid_ref[k], high_ref[which], low_ref[which])
        subs = []
        for lanes in (slice(0, LANES), slice(LANES, 2 * LANES)):
            top, low = value[: block // 2, lanes], value[block // 2 :, lanes]
            subs.append(jnp.where(left, top, pltpu.roll(low, HALF, 1)))
            subs.append(jnp.where(left, pltpu.roll(top, HALF, 1), low))
        for out_ref, value in zip(out_refs, subs):
            out_ref[k] = value
        return carry

    lax.fori_loop(0, OUTER // 2, family, 0)


def bins_kernel(info_ref, flip_ref, *refs):
    bins_refs, out_ref, turn_ref = refs[:-2], refs[-2], refs[-1]
    step = pl.program_id(0)
    sub = bins_refs[0].shape[1]
    parity = info_ref[0]
    upper = info_ref[1]
    dests = out_ref.shape[0]
    width = out_ref.shape[3]
    zero = parity == 0
    high_side = upper == 1
    flat_refs = [ref.reshape(LANES * sub, LANES) for ref in bins_refs]
    for c in range(sub):
        kappa = step * sub + c
        mirrored = (OUTER - kappa) % OUTER
        for part, ref in enumerate(flat_refs):
            turn_ref[c % 2, part * LANES : (part + 1) * LANES] = (
                ref[pl.ds(c, LANES, stride=sub), :].astype(jnp.float32).T
            )

        def column(at):
            return turn_ref[c % 2, pl.ds(at, width, stride=OUTER), :]

        ahead = [column(jnp.where(zero & high_side, OUTER // 2, parity))]
        back = [column(jnp.where(zero, jnp.where(high_side, 0, OUTER // 2), OUTER - parity))]
        for dest in range(1, dests):
            ahead.append(column(2 * dest + parity))
            back.append(column(OUTER - 2 * dest - parity))
        mixed = jnp.concatenate([ahead[0]] + back, 0)
        high = jnp.floor(mixed * 0.125)
        pair = jnp.concatenate([high.astype(jnp.bfloat16), (mixed - high * 8.0).astype(jnp.bfloat16)], 1)
        flipped = dot_f32(pair, flip_ref[jnp.minimum(kappa, 1)])
        turn0 = zero & high_side
        turn1 = jnp.logical_not(zero & jnp.logical_not(high_side))
        out_ref[0, 0, jnp.where(turn0, mirrored, kappa)] = jnp.where(turn0, flipped[:width], ahead[0])
        out_ref[0, 1, jnp.where(turn1, mirrored, kappa)] = jnp.where(
            turn1, flipped[width : 2 * width], back[0]
        )
        for dest in range(1, dests):
            out_ref[dest, 0, kappa] = ahead[dest]
            out_ref[dest, 1, mirrored] = flipped[(dest + 1) * width : (dest + 2) * width]


def band_kernel(
    extent, half_chunk, with_edge, info_ref, x_ref, bins0_ref, bins1_ref, turn_ref, high_ref, low_ref,
    fx_ref, *refs,
):
    if with_edge:
        sums_ref, edge_ref, mid_ref, power_ref, part_ref = refs
    else:
        sums_ref, mid_ref, power_ref, part_ref = refs
    sub = half_chunk
    offset = info_ref[0]
    flipped = info_ref[1]
    hollow = (info_ref[2] == 1) if sub == 0 else False
    per_slab = x_ref.shape[3] // HALF
    even8 = lax.broadcasted_iota(jnp.int32, (8, LANES), 1) % HALF < SUB

    def tile(step, carry):
        start = pl.multiple_of(step * 8, 8)
        cells = []
        for a in range(OUTER):
            rows = pl.ds((a % per_slab) * HALF + start, 8)
            q = x_ref[a // per_slab, 0, 0, rows, :]
            u = x_ref[a // per_slab, 1, 0, rows, :]
            real = jnp.where(even8, q, pltpu.roll(u, SUB, 1))
            imag = jnp.where(even8, pltpu.roll(q, LANES - SUB, 1), u)
            cells.append((real, imag))
        waves = complex_fft(cells)
        turns = {1: (turn_ref[0, pl.ds(start, 8), :], turn_ref[1, pl.ds(start, 8), :])}
        mid_ref[0, pl.ds(start, 8), :] = waves[0][0]
        mid_ref[0, pl.ds(HALF + start, 8), :] = waves[0][1]
        for k in range(1, OUTER):
            if k not in turns:
                (ar, ai), (br, bi) = turns[k // 2], turns[k - k // 2]
                turns[k] = (ar * br - ai * bi, ar * bi + ai * br)
            cosine, sine = turns[k]
            real, imag = waves[k]
            mid_ref[k, pl.ds(start, 8), :] = real * cosine - imag * sine
            mid_ref[k, pl.ds(HALF + start, 8), :] = real * sine + imag * cosine
        return carry

    lax.fori_loop(0, HALF // 8, tile, 0)

    fx = fx_ref[0]
    lane = lax.broadcasted_iota(jnp.int32, (SUB, LANES), 1)
    slot = lax.broadcasted_iota(jnp.int32, (SUB, LANES), 0)
    keep = jnp.where((slot == 0) & hollow, 0.0, 1.0) if sub == 0 else 1.0
    inv_area = 1.0 / (extent * extent)
    group_iota = lax.broadcasted_iota(jnp.int32, (GROUPS, LANES), 0).astype(jnp.float32).astype(jnp.bfloat16)
    low_iota = lax.broadcasted_iota(jnp.int32, (LOWS, LANES), 0).astype(jnp.float32).astype(jnp.bfloat16)
    width = bins0_ref.shape[3]
    near = SUB // width
    one = jnp.ones((LOWS, LANES), jnp.bfloat16)
    none = jnp.zeros((LOWS, LANES), jnp.bfloat16)
    empty = jnp.zeros((GROUPS, LANES), jnp.bfloat16)
    begin0 = sub * near
    begin1 = (1 - sub) * near

    def batch(step, acc):
        turned_rows = []
        for member in range(BATCH):
            flat = mid_ref[BATCH * step + member].T
            turned_rows.append(jnp.concatenate([flat[:HALF], flat[HALF:]], 1))
        spectra = three_pass(jnp.concatenate(turned_rows, 0), high_ref[...], low_ref[...])
        weighted, lows = [], []
        for member in range(BATCH):
            k = BATCH * step + member
            spectrum = spectra[member * HALF : (member + 1) * HALF]
            if with_edge:
                edge_ref[sub, k, 0:1, :] = spectrum[0:1, :]
                edge_ref[sub, k, 1:2, :] = spectrum[SUB : SUB + 1, :]
            q_real, q_imag = spectrum[:SUB, :LANES], spectrum[:SUB, LANES:]
            u_real, u_imag = spectrum[SUB:, :LANES], spectrum[SUB:, LANES:]
            row = lane * OUTER + k
            fy = jnp.where(row >= extent // 2, row - extent, row).astype(jnp.float32)
            radius = jnp.maximum(fx * fx + fy * fy, 1.0)
            cos_twice = (fx * fx - fy * fy) / radius
            sin_twice = 2.0 * fx * fy / radius

            def powers(sine, which):
                e_real = cos_twice * q_real + sine * u_real
                e_imag = cos_twice * q_imag + sine * u_imag
                b_real = cos_twice * u_real - sine * q_real
                b_imag = cos_twice * u_imag - sine * q_imag
                power_ref[member, which, 0] = (e_real * e_real + e_imag * e_imag) * inv_area * keep
                power_ref[member, which, 1] = (b_real * b_real + b_imag * b_imag) * inv_area * keep
                power_ref[member, which, 2] = (e_real * b_real + e_imag * b_imag) * inv_area * keep

            other = 0
            if member == 0:
                other = jnp.where(k == 0, 1, 0)
                powers(sin_twice, jnp.where(k == 0, 1 - flipped, 0))

                @pl.when(k == 0)
                def _():
                    powers(jnp.where(row == extent // 2, -sin_twice, sin_twice), flipped)

            else:
                powers(sin_twice, 0)

            for index, (bins_ref, begin, count) in enumerate(
                ((bins0_ref, begin0, near), (bins1_ref, begin1, near + 1))
            ):
                for source in range(count):
                    at = min(begin + source, bins_ref.shape[0] - 1)
                    value = bins_ref[at, 0, k]
                    high = jnp.floor(value * (1.0 / LOWS))
                    rows = slice(source * width, (source + 1) * width)
                    part_ref[member, index, 0, rows] = high
                    part_ref[member, index, 1, rows] = value - high * LOWS

            for i in range(SUB):
                mirror = offset - HALF + SUB - i
                for index, at, source in ((0, i, 0), (1, mirror, other)):
                    high = part_ref[member, index, 0, pl.ds(at, 1), :]
                    low = part_ref[member, index, 1, pl.ds(at, 1), :]
                    high = jnp.broadcast_to(high, (GROUPS, LANES)).astype(jnp.bfloat16)
                    low = jnp.broadcast_to(low, (LOWS, LANES)).astype(jnp.bfloat16)
                    hot = high == group_iota
                    column = []
                    for kind in range(3):
                        power = power_ref[member, source, kind, pl.ds(i, 1), :]
                        power = jnp.broadcast_to(power, (GROUPS, LANES)).astype(jnp.bfloat16)
                        column.append(jnp.where(hot, power, empty))
                    weighted.append(jnp.concatenate(column, 0))
                    lows.append(jnp.where(low == low_iota, one, none))
        return acc + dot_f32(
            jnp.concatenate(weighted, 1), jnp.concatenate(lows, 1), (((1,), (1,)), ((), ()))
        )

    sums_ref[0] = lax.fori_loop(0, OUTER // BATCH, batch, jnp.zeros((3 * GROUPS, LOWS), jnp.float32))


def summed(array, axis):
    distance = 0
    while 1 << distance < lax.axis_size(axis):
        array = array + partner(array, axis, distance)
        distance += 1
    return array


def edge_sums(edge, bins_left, bins_right, extent):
    flat = edge.transpose(1, 2, 0).reshape(2, 2, extent)
    back = jnp.roll(flat[:, :, ::-1], 1, axis=2)
    q_real, q_imag, u_real, u_imag = [
        jnp.stack(pair)
        for m in range(2)
        for pair in (
            (0.5 * (flat[m, 0] + back[m, 0]), 0.5 * (flat[m, 1] + back[m, 1])),
            (0.5 * (flat[m, 1] - back[m, 1]), 0.5 * (back[m, 0] - flat[m, 0])),
        )
    ]
    freq_y = signed_float(lax.iota(jnp.int32, extent), extent)[None, :]
    freq_x = jnp.array([0.0, -extent // 2], jnp.float32)[:, None]
    left = bins_left.T.reshape(extent)
    right = jnp.roll(bins_right.T.reshape(extent)[::-1], 1)
    bins = jnp.stack([left, right]).astype(jnp.int32)
    return band_terms((q_real, q_imag, u_real, u_imag), freq_y, freq_x, bins, NBINS, extent)


def on_device_fast(maps, mask, bins):
    extent = bins.shape[0]
    columns = bins.shape[1]
    count = maps.shape[1]
    slabs = lax.axis_size("rows")
    reps = lax.axis_size("rep")
    slab_index = lax.axis_index("rows")
    member = lax.axis_index("rep")
    pair_bit = member % 2
    half_slabs = slabs // 2
    first, family, natural = host_tables(extent)
    row_high, row_low = split_table(np.stack([first, family]))
    col_high, col_low = split_table(natural)

    flips = np.zeros((2, 2 * LANES, LANES))
    for k in range(LANES):
        flips[0, k, -k % LANES] = 8.0
        flips[0, LANES + k, -k % LANES] = 1.0
        flips[1, k, LANES - 1 - k] = 8.0
        flips[1, LANES + k, LANES - 1 - k] = 1.0
    info = jnp.stack([pair_bit, (slab_index >= half_slabs).astype(jnp.int32)])
    sub = 8
    width = columns // OUTER
    sent_bins = pl.pallas_call(
        bins_kernel,
        grid=(OUTER // sub,),
        in_specs=[
            pl.BlockSpec(memory_space=pltpu.SMEM),
            pl.BlockSpec((2, 2 * LANES, LANES), lambda i: (0, 0, 0)),
        ]
        + [
            pl.BlockSpec((LANES, sub, LANES), lambda i, part=part: (0, i, part))
            for part in range(columns // LANES)
        ],
        out_specs=pl.BlockSpec((slabs, 2, OUTER, width, LANES), lambda i: (0, 0, 0, 0, 0)),
        out_shape=jax.ShapeDtypeStruct((slabs, 2, OUTER, width, LANES), jnp.float32),
        scratch_shapes=[pltpu.VMEM((2, columns, LANES), jnp.float32)],
        cost_estimate=pl.CostEstimate(flops=5 * 10**9, transcendentals=0, bytes_accessed=12 * 2**20),
        name="bins_prep",
    )(info, jnp.asarray(flips, jnp.bfloat16), *[bins.reshape(LANES, OUTER, columns)] * (columns // LANES))
    got_bins = lax.all_to_all(sent_bins, "rows", split_axis=0, concat_axis=0, tiled=True)

    block = min(LANES, count)
    k1 = np.arange(OUTER // 2)[:, None]
    angles = 2 * np.pi * (k1 * np.arange(LANES)[None, :] % extent) / extent
    turns = jnp.asarray(np.stack([np.cos(angles), -np.sin(angles)]), jnp.float32)
    table_spec = pl.BlockSpec((2, 2 * LANES, 2 * LANES), lambda i: (0, 0, 0))
    piece = jax.ShapeDtypeStruct((2 * slabs, count // 2, LANES), jnp.float32)
    piece_spec = pl.BlockSpec((2 * slabs, block // 2, LANES), lambda i: (0, i, 0))
    pieces = pl.pallas_call(
        row_kernel,
        grid=(count // block,),
        in_specs=[
            pl.BlockSpec((1, block, extent), lambda i: (0, i, 0)),
            pl.BlockSpec((block, extent), lambda i: (i, 0)),
            pl.BlockSpec(turns.shape, lambda i: (0, 0, 0)),
            table_spec,
            table_spec,
        ],
        out_specs=[piece_spec] * (LANES // SUB),
        out_shape=[piece] * (LANES // SUB),
        scratch_shapes=[pltpu.VMEM((OUTER // 2, block, 2 * LANES), jnp.float32)],
        cost_estimate=pl.CostEstimate(flops=12 * 10**9, transcendentals=0, bytes_accessed=24 * 2**20),
        name="row_fft",
    )(maps, mask, turns, row_high, row_low)

    groups = [
        [row * reps + z for row in range(slabs) for z in (2 * sky, 2 * sky + 1)]
        for sky in range(reps // 2)
    ]
    fam = 2 * slab_index + pair_bit
    angles = np.arange(HALF)[:, None] + HALF * (np.arange(LANES)[None, :] >= HALF)
    angles = 2 * np.pi * angles / extent
    spin = jnp.asarray(np.stack([np.cos(angles), -np.sin(angles)]), jnp.float32)
    slots = lax.iota(jnp.int32, HALF)
    zero = (fam == 0).astype(jnp.int32)
    total = None
    before = got_bins
    for number, piece in enumerate(pieces):
        chunk, half_chunk = number // 2, number % 2
        piece, before = lax.optimization_barrier((piece, before))
        got = lax.all_to_all(
            piece, ("rows", "rep"), split_axis=0, concat_axis=0, tiled=True,
            axis_index_groups=groups,
        )
        before = got
        got = got.reshape(slabs, 2, -1, count // 2, LANES)
        subs = got.shape[2]
        first_col = OUTER * slots if chunk == 0 else OUTER // 2 + OUTER * (HALF - 1 - slots)
        col = jnp.where(fam == 0, first_col, fam + OUTER * (slots + HALF * chunk))
        col = col[half_chunk * SUB : (half_chunk + 1) * SUB]
        fx = jnp.broadcast_to(signed_float(col, extent).reshape(subs, SUB, 1), (subs, SUB, LANES))
        with_edge = number == 0
        if chunk == 0:
            info = jnp.stack([HALF - 1 + zero, jnp.int32(1), zero])
        else:
            info = jnp.stack([jnp.int32(HALF - 1), 1 - zero, jnp.int32(0)])
        if number == 1:
            info, special = lax.optimization_barrier((info, special))
        bin_block = (half_slabs, 1, OUTER, width, LANES)
        edge_shape = (subs, OUTER, 2, 2 * LANES)
        sums_shape = (subs, 3 * GROUPS, LOWS)
        band_call = pl.pallas_call(
            functools.partial(band_kernel, extent, half_chunk, with_edge),
            grid=(subs,),
            in_specs=[
                pl.BlockSpec(memory_space=pltpu.SMEM),
                pl.BlockSpec((slabs, 2, 1, count // 2, LANES), lambda i: (0, 0, i, 0, 0)),
                pl.BlockSpec(bin_block, lambda i, at=chunk: (at, 0, 0, 0, 0)),
                pl.BlockSpec(bin_block, lambda i, at=1 - chunk: (at, 1, 0, 0, 0)),
                pl.BlockSpec(spin.shape, lambda i: (0, 0, 0)),
                pl.BlockSpec(col_high.shape, lambda i: (0, 0)),
                pl.BlockSpec(col_low.shape, lambda i: (0, 0)),
                pl.BlockSpec((1, SUB, LANES), lambda i: (i, 0, 0)),
            ],
            out_specs=[pl.BlockSpec((1, 3 * GROUPS, LOWS), lambda i: (i, 0, 0))]
            + [pl.BlockSpec(edge_shape, lambda i: (0, 0, 0, 0))] * with_edge,
            out_shape=[jax.ShapeDtypeStruct(sums_shape, jnp.float32)]
            + [jax.ShapeDtypeStruct(edge_shape, jnp.float32)] * with_edge,
            scratch_shapes=[
                pltpu.VMEM((OUTER, LANES, LANES), jnp.float32),
                pltpu.VMEM((BATCH, 2, 3, SUB, LANES), jnp.float32),
                pltpu.VMEM((BATCH, 2, 2, SUB + width, LANES), jnp.float32),
            ],
            compiler_params=pltpu.CompilerParams(vmem_limit_bytes=48 * 2**20),
            cost_estimate=pl.CostEstimate(flops=10**10, transcendentals=0, bytes_accessed=4 * 2**20),
            name="band_sums",
        )
        out = band_call(info, got, got_bins, got_bins, spin, col_high, col_low, fx)
        sums = out[0].sum(0)
        total = sums if total is None else total + sums
        if with_edge:
            special = edge_sums(
                out[1][0], got_bins[0, 0, :, 0], got_bins[half_slabs, 1, :, 0], extent
            )
            special = jnp.where(fam == 0, special, 0.0)
    partial_sums = total.reshape(3, NBINS) + special
    auto = NBINS / (extent * extent)
    cross = math.sqrt(auto)
    factors = jnp.array([auto, auto, cross], jnp.float32)[:, None]
    own = summed(partial_sums, "rows")

    def from_rep(shift):
        if shift == 0:
            return own
        return lax.ppermute(own, "rep", [(i, i ^ shift) for i in range(reps)])

    skies = [
        (from_rep(2 * shift) + from_rep(2 * shift + 1)) * factors for shift in range(reps // 2)
    ]
    stacked = jnp.stack(skies)
    order = lax.iota(jnp.int32, len(skies)) ^ (member // 2)
    return jnp.take(stacked, order, axis=0) if len(skies) > 2 else jnp.where(
        member // 2 == 0, stacked, stacked[::-1]
    )


def solution(mesh):
    in_specs = (P("rep", "rows", None), P("rows", None), P(None, "rows"))
    out_specs = P()

    def on_any(maps, mask, bins):
        extent = bins.shape[0]
        families = 2 * lax.axis_size("rows")
        if extent == OUTER * LANES and families == OUTER // 2 and NBINS == GROUPS * LOWS:
            return on_device_fast(maps, mask, bins)
        return on_device(maps, mask, bins)

    return jax.shard_map(
        on_any, mesh=mesh, in_specs=in_specs, out_specs=out_specs, check_vma=False
    )
```

```python
import functools
import math

import jax
import jax.numpy as jnp
import numpy as np
from jax import lax
from jax.experimental import pallas as pl
from jax.experimental.pallas import tpu as pltpu
from jax.sharding import PartitionSpec as P


NBINS = 1024


precise = lax.Precision.HIGHEST


def partner(array, axis, distance):
    return lax.ppermute(array, axis, [(i, i ^ 1 << distance) for i in range(lax.axis_size(axis))])


def dft_table(count_a, count_b, period):
    first = lax.iota(jnp.int32, count_a)[:, None]
    second = lax.iota(jnp.int32, count_b)[None, :]
    angles = (first * second % period).astype(jnp.float32) * (2.0 * math.pi / period)
    return (jnp.cos(angles), -jnp.sin(angles))


def split_length(length):
    outer_len = 2 ** ((length.bit_length() - 1) // 2)
    return (outer_len, length // outer_len)


def complex_apply(form, real_part, imag_part, table_cos, table_sin):

    def product(left, right):
        return jnp.einsum(form, left, right, precision=precise)

    return (
        product(real_part, table_cos) - product(imag_part, table_sin),
        product(real_part, table_sin) + product(imag_part, table_cos),
    )


def twiddled(real_part, imag_part, table_cos, table_sin):
    return (
        real_part * table_cos - imag_part * table_sin,
        real_part * table_sin + imag_part * table_cos,
    )


def row_transform(values):
    count, length = values.shape
    outer_len, inner_len = split_length(length)
    outer_cos, outer_sin = dft_table(outer_len, outer_len, outer_len)
    inner_cos, inner_sin = dft_table(inner_len, inner_len, inner_len)
    turn_cos, turn_sin = dft_table(outer_len, inner_len, length)
    shaped = values.reshape(count, outer_len, inner_len)
    first_real = jnp.einsum("yan,ak->ykn", shaped, outer_cos, precision=precise)
    first_imag = jnp.einsum("yan,ak->ykn", shaped, outer_sin, precision=precise)
    mid_real, mid_imag = twiddled(first_real, first_imag, turn_cos, turn_sin)
    last_real, last_imag = complex_apply("ykn,nm->ymk", mid_real, mid_imag, inner_cos, inner_sin)
    return (last_real.reshape(count, length), last_imag.reshape(count, length))


def column_transform(pieces):
    real_part, imag_part = pieces
    length, groups, width = real_part.shape
    outer_len, inner_len = split_length(length)
    outer_cos, outer_sin = dft_table(outer_len, outer_len, outer_len)
    inner_cos, inner_sin = dft_table(inner_len, inner_len, inner_len)
    turn_cos, turn_sin = dft_table(outer_len, inner_len, length)
    shaped_real = real_part.reshape(outer_len, inner_len, groups, width)
    shaped_imag = imag_part.reshape(outer_len, inner_len, groups, width)
    first_real, first_imag = complex_apply(
        "anbc,ak->knbc", shaped_real, shaped_imag, outer_cos, outer_sin
    )
    mid_real, mid_imag = twiddled(
        first_real, first_imag, turn_cos[:, :, None, None], turn_sin[:, :, None, None]
    )
    last_real, last_imag = complex_apply("knbc,nm->mkbc", mid_real, mid_imag, inner_cos, inner_sin)
    return (last_real.reshape(length, groups, width), last_imag.reshape(length, groups, width))


def signed_float(indices, extent):
    return jnp.where(indices >= extent // 2, indices - extent, indices).astype(jnp.float32)


def band_terms(fields, freq_y, freq_x, bin_block, nbins_count, extent):
    q_real, q_imag, u_real, u_imag = fields
    radius = jnp.maximum(freq_x * freq_x + freq_y * freq_y, 1.0)
    cos_twice = (freq_x * freq_x - freq_y * freq_y) / radius
    sin_twice = 2.0 * freq_x * freq_y / radius
    e_real = cos_twice * q_real + sin_twice * u_real
    e_imag = cos_twice * q_imag + sin_twice * u_imag
    b_real = -sin_twice * q_real + cos_twice * u_real
    b_imag = -sin_twice * q_imag + cos_twice * u_imag
    inv_area = 1.0 / (extent * extent)
    powers = jnp.stack(
        [
            (e_real * e_real + e_imag * e_imag) * inv_area,
            (b_real * b_real + b_imag * b_imag) * inv_area,
            (e_real * b_real + e_imag * b_imag) * inv_area,
        ]
    ).astype(jnp.bfloat16)
    bit_count = nbins_count.bit_length() - 1
    high_count = 2 ** max(bit_count // 2 - 1, 0)
    low_count = nbins_count // high_count
    high_part = bin_block // low_count
    low_part = bin_block % low_count
    high_hot = (high_part[None] == lax.iota(jnp.int32, high_count)[:, None, None]).astype(
        jnp.bfloat16
    )
    weighted = (powers[:, None] * high_hot[None]).reshape(3 * high_count, -1)
    low_hot = (low_part[None] == lax.iota(jnp.int32, low_count)[:, None, None]).astype(jnp.bfloat16)
    low_hot = low_hot.reshape(low_count, -1)
    sums = lax.dot_general(
        weighted, low_hot, (((1,), (1,)), ((), ())), preferred_element_type=jnp.float32
    )
    return sums.reshape(3, nbins_count)


def on_device(maps, mask, bins):
    extent = bins.shape[0]
    columns = bins.shape[1]
    count = maps.shape[1]
    slab_index = lax.axis_index("rows")
    member = lax.axis_index("rep")
    pair_bit = member % 2
    field = maps[0] * mask.astype(jnp.float32)
    row_real, row_imag = row_transform(field)
    half_rows = extent // 2
    slabs = (
        row_real.reshape(count, extent // columns, columns),
        row_imag.reshape(count, extent // columns, columns),
    )
    spec_real, spec_imag = column_transform(
        (
            lax.all_to_all(slabs[0], "rows", split_axis=1, concat_axis=0, tiled=True),
            lax.all_to_all(slabs[1], "rows", split_axis=1, concat_axis=0, tiled=True),
        )
    )
    spec_real = spec_real.reshape(extent, columns)
    spec_imag = spec_imag.reshape(extent, columns)
    kept_real = lax.dynamic_slice_in_dim(spec_real, pair_bit * half_rows, half_rows, 0)
    kept_imag = lax.dynamic_slice_in_dim(spec_imag, pair_bit * half_rows, half_rows, 0)
    sent_real = lax.dynamic_slice_in_dim(spec_real, (1 - pair_bit) * half_rows, half_rows, 0)
    sent_imag = lax.dynamic_slice_in_dim(spec_imag, (1 - pair_bit) * half_rows, half_rows, 0)
    got_real, got_imag = partner((sent_real, sent_imag), "rep", 0)
    is_first = pair_bit == 0
    fields = (
        jnp.where(is_first, kept_real, got_real),
        jnp.where(is_first, kept_imag, got_imag),
        jnp.where(is_first, got_real, kept_real),
        jnp.where(is_first, got_imag, kept_imag),
    )
    own_bins = lax.dynamic_slice_in_dim(bins, pair_bit * half_rows, half_rows, 0)

    def frequency_of(offset, height):
        rows_here = lax.iota(jnp.int32, height)[:, None] + offset + pair_bit * half_rows
        cols_here = lax.iota(jnp.int32, columns)[None, :] + slab_index * columns
        return (rows_here, cols_here)

    block = min(256, half_rows)
    blocks = half_rows // block
    stacked = tuple((part.reshape(blocks, block, columns) for part in fields))
    bin_blocks = own_bins.reshape(blocks, block, columns)

    def accumulate(running, items):
        block_index, parts, bin_block = items
        rows_here, cols_here = frequency_of(block_index * block, block)
        term = band_terms(
            parts,
            signed_float(rows_here, extent),
            signed_float(cols_here, extent),
            bin_block,
            NBINS,
            extent,
        )
        return (running + term, None)

    partial_sums, _ = lax.scan(
        accumulate,
        jnp.zeros((3, NBINS), jnp.float32),
        (lax.iota(jnp.int32, blocks), stacked, bin_blocks),
    )
    sims_count = lax.axis_size("rep") // 2
    slot = (lax.iota(jnp.int32, sims_count) == member // 2).astype(jnp.float32)[:, None, None]
    totals = lax.psum(slot * partial_sums[None], ("rows", "rep"))
    auto = NBINS / (extent * extent)
    cross = math.sqrt(auto)
    factors = jnp.array([auto, auto, cross], jnp.float32)[None, :, None]
    return totals * factors


LANES = 128
OUTER = 32
HALF = LANES // 2
SUB = LANES // 4
BATCH = 8
GROUPS = 16
LOWS = 64


def fft_wave(index, size):
    return (math.cos(2 * math.pi * index / size), -math.sin(2 * math.pi * index / size))


def turned(value, index, size):
    real, imag = value
    if index == 0:
        return value
    if 4 * index == size:
        return (imag, -real)
    cosine, sine = fft_wave(index, size)
    if 8 * index == size:
        return ((real + imag) * cosine, (imag - real) * cosine)
    if 8 * index == 3 * size:
        return ((imag - real) * -cosine, (real + imag) * cosine)
    return (real * cosine - imag * sine, real * sine + imag * cosine)


def real_fft(values):
    size = len(values)
    if size == 2:
        return [(values[0] + values[1], None), (values[0] - values[1], None)]
    even = real_fft(values[0::2])
    odd = real_fft(values[1::2])
    half = size // 2
    out = [None] * (half + 1)
    out[0] = (even[0][0] + odd[0][0], None)
    out[half] = (even[0][0] - odd[0][0], None)
    quarter = size // 4
    out[quarter] = (even[quarter][0], -odd[quarter][0])
    for k in range(1, quarter):
        real, imag = turned(odd[k], k, size)
        out[k] = (even[k][0] + real, even[k][1] + imag)
        out[half - k] = (even[k][0] - real, imag - even[k][1])
    return out


def complex_fft(values):
    size = len(values)
    if size == 1:
        return values
    even = complex_fft(values[0::2])
    odd = complex_fft(values[1::2])
    half = size // 2
    out = [None] * size
    for k in range(half):
        real, imag = turned(odd[k], k, size)
        out[k] = (even[k][0] + real, even[k][1] + imag)
        out[k + half] = (even[k][0] - real, even[k][1] - imag)
    return out


def wave_matrix(angles):
    cosine, sine = np.cos(angles), np.sin(angles)
    return cosine, sine


def host_tables(extent):
    b = np.arange(LANES)[:, None]
    k = np.arange(LANES)[None, :]
    cosine, sine = wave_matrix(2 * np.pi * (b * k % LANES) / LANES)
    natural = np.concatenate(
        [np.concatenate([cosine, -sine], 1), np.concatenate([sine, cosine], 1)], 0
    )
    first = np.zeros((2 * LANES, 2 * LANES))
    first[:LANES, :HALF] = cosine[:, :HALF]
    first[:LANES, LANES : LANES + HALF] = -sine[:, :HALF]
    first[:LANES, LANES] = 1.0 - 2.0 * (np.arange(LANES) % 2)
    freq = OUTER // 2 + OUTER * (HALF - 1 - np.arange(HALF)[None, :])
    cosine, sine = wave_matrix(2 * np.pi * (b * freq % extent) / extent)
    first[LANES:, HALF:LANES] = cosine
    first[LANES:, LANES + HALF :] = -sine
    order = np.concatenate(
        [part + SUB * s + np.arange(SUB) for s in range(LANES // SUB) for part in (0, LANES)]
    )
    rows = np.concatenate([part + HALF * h + np.arange(HALF) for h in range(2) for part in (0, LANES)])
    return first[:, order], natural[:, order], natural[rows]


def split_table(table):
    table = jnp.asarray(table, jnp.float32)
    high = table.astype(jnp.bfloat16)
    return high, (table - high.astype(jnp.float32)).astype(jnp.bfloat16)


def split_value(value):
    high = value.astype(jnp.bfloat16)
    return high, (value - high.astype(jnp.float32)).astype(jnp.bfloat16)


def dot_f32(left, right, dims=(((1,), (0,)), ((), ()))):
    return lax.dot_general(left, right, dims, preferred_element_type=jnp.float32)


def three_pass(value, table_high, table_low):
    high, low = split_value(value)
    return dot_f32(high, table_high) + (dot_f32(low, table_high) + dot_f32(high, table_low))


def row_kernel(
    map_ref, mask_ref, turn_ref, high_ref, low_ref, *refs
):
    out_refs, mid_ref = refs[:-1], refs[-1]
    block = map_ref.shape[1]
    left = lax.broadcasted_iota(jnp.int32, (block // 2, LANES), 1) < HALF

    def tile(step, carry):
        start = pl.multiple_of(step * 8, 8)
        cells = []
        for a in range(OUTER):
            lanes = pl.ds(a * LANES, LANES)
            weight = mask_ref[pl.ds(start, 8), lanes].astype(jnp.float32)
            cells.append(map_ref[0, pl.ds(start, 8), lanes] * weight)
        waves = real_fft(cells)
        half = OUTER // 2
        mid_ref[0, pl.ds(start, 8), 0:LANES] = waves[0][0]
        mid_ref[0, pl.ds(start, 8), LANES : 2 * LANES] = waves[half][0]
        for k in range(1, half):
            real, imag = waves[k]
            cosine = turn_ref[0, k : k + 1, :]
            sine = turn_ref[1, k : k + 1, :]
            mid_ref[k, pl.ds(start, 8), 0:LANES] = real * cosine - imag * sine
            mid_ref[k, pl.ds(start, 8), LANES : 2 * LANES] = real * sine + imag * cosine
        return carry

    lax.fori_loop(0, block // 8, tile, 0)

    def family(k, carry):
        which = jnp.minimum(k, 1)
        value = three_pass(mid_ref[k], high_ref[which], low_ref[which])
        subs = []
        for lanes in (slice(0, LANES), slice(LANES, 2 * LANES)):
            top, low = value[: block // 2, lanes], value[block // 2 :, lanes]
            subs.append(jnp.where(left, top, pltpu.roll(low, HALF, 1)))
            subs.append(jnp.where(left, pltpu.roll(top, HALF, 1), low))
        for out_ref, value in zip(out_refs, subs):
            out_ref[k] = value
        return carry

    lax.fori_loop(0, OUTER // 2, family, 0)


def bins_kernel(info_ref, flip_ref, *refs):
    bins_refs, out_ref, turn_ref = refs[:-2], refs[-2], refs[-1]
    step = pl.program_id(0)
    sub = bins_refs[0].shape[1]
    parity = info_ref[0]
    upper = info_ref[1]
    dests = out_ref.shape[0]
    width = out_ref.shape[3]
    zero = parity == 0
    high_side = upper == 1
    flat_refs = [ref.reshape(LANES * sub, LANES) for ref in bins_refs]
    for c in range(sub):
        kappa = step * sub + c
        mirrored = (OUTER - kappa) % OUTER
        for part, ref in enumerate(flat_refs):
            turn_ref[c % 2, part * LANES : (part + 1) * LANES] = (
                ref[pl.ds(c, LANES, stride=sub), :].astype(jnp.float32).T
            )

        def column(at):
            return turn_ref[c % 2, pl.ds(at, width, stride=OUTER), :]

        ahead = [column(jnp.where(zero & high_side, OUTER // 2, parity))]
        back = [column(jnp.where(zero, jnp.where(high_side, 0, OUTER // 2), OUTER - parity))]
        for dest in range(1, dests):
            ahead.append(column(2 * dest + parity))
            back.append(column(OUTER - 2 * dest - parity))
        mixed = jnp.concatenate([ahead[0]] + back, 0)
        high = jnp.floor(mixed * 0.125)
        pair = jnp.concatenate([high.astype(jnp.bfloat16), (mixed - high * 8.0).astype(jnp.bfloat16)], 1)
        flipped = dot_f32(pair, flip_ref[jnp.minimum(kappa, 1)])
        turn0 = zero & high_side
        turn1 = jnp.logical_not(zero & jnp.logical_not(high_side))
        out_ref[0, 0, jnp.where(turn0, mirrored, kappa)] = jnp.where(turn0, flipped[:width], ahead[0])
        out_ref[0, 1, jnp.where(turn1, mirrored, kappa)] = jnp.where(
            turn1, flipped[width : 2 * width], back[0]
        )
        for dest in range(1, dests):
            out_ref[dest, 0, kappa] = ahead[dest]
            out_ref[dest, 1, mirrored] = flipped[(dest + 1) * width : (dest + 2) * width]


def band_kernel(
    extent, half_chunk, with_edge, info_ref, x_ref, bins0_ref, bins1_ref, turn_ref, high_ref, low_ref,
    fx_ref, *refs,
):
    if with_edge:
        sums_ref, edge_ref, mid_ref, power_ref, part_ref = refs
    else:
        sums_ref, mid_ref, power_ref, part_ref = refs
    sub = half_chunk
    offset = info_ref[0]
    flipped = info_ref[1]
    hollow = (info_ref[2] == 1) if sub == 0 else False
    per_slab = x_ref.shape[3] // HALF
    even8 = lax.broadcasted_iota(jnp.int32, (8, LANES), 1) % HALF < SUB

    def tile(step, carry):
        start = pl.multiple_of(step * 8, 8)
        cells = []
        for a in range(OUTER):
            rows = pl.ds((a % per_slab) * HALF + start, 8)
            q = x_ref[a // per_slab, 0, 0, rows, :]
            u = x_ref[a // per_slab, 1, 0, rows, :]
            real = jnp.where(even8, q, pltpu.roll(u, SUB, 1))
            imag = jnp.where(even8, pltpu.roll(q, LANES - SUB, 1), u)
            cells.append((real, imag))
        waves = complex_fft(cells)
        turns = {1: (turn_ref[0, pl.ds(start, 8), :], turn_ref[1, pl.ds(start, 8), :])}
        mid_ref[0, pl.ds(start, 8), :] = waves[0][0]
        mid_ref[0, pl.ds(HALF + start, 8), :] = waves[0][1]
        for k in range(1, OUTER):
            if k not in turns:
                (ar, ai), (br, bi) = turns[k // 2], turns[k - k // 2]
                turns[k] = (ar * br - ai * bi, ar * bi + ai * br)
            cosine, sine = turns[k]
            real, imag = waves[k]
            mid_ref[k, pl.ds(start, 8), :] = real * cosine - imag * sine
            mid_ref[k, pl.ds(HALF + start, 8), :] = real * sine + imag * cosine
        return carry

    lax.fori_loop(0, HALF // 8, tile, 0)

    fx = fx_ref[0]
    lane = lax.broadcasted_iota(jnp.int32, (SUB, LANES), 1)
    slot = lax.broadcasted_iota(jnp.int32, (SUB, LANES), 0)
    keep = jnp.where((slot == 0) & hollow, 0.0, 1.0) if sub == 0 else 1.0
    inv_area = 1.0 / (extent * extent)
    group_iota = lax.broadcasted_iota(jnp.int32, (GROUPS, LANES), 0).astype(jnp.float32).astype(jnp.bfloat16)
    low_iota = lax.broadcasted_iota(jnp.int32, (LOWS, LANES), 0).astype(jnp.float32).astype(jnp.bfloat16)
    width = bins0_ref.shape[3]
    near = SUB // width
    one = jnp.ones((LOWS, LANES), jnp.bfloat16)
    none = jnp.zeros((LOWS, LANES), jnp.bfloat16)
    empty = jnp.zeros((GROUPS, LANES), jnp.bfloat16)
    begin0 = sub * near
    begin1 = (1 - sub) * near

    def batch(step, acc):
        turned_rows = []
        for member in range(BATCH):
            flat = mid_ref[BATCH * step + member].T
            turned_rows.append(jnp.concatenate([flat[:HALF], flat[HALF:]], 1))
        spectra = three_pass(jnp.concatenate(turned_rows, 0), high_ref[...], low_ref[...])
        weighted, lows = [], []
        for member in range(BATCH):
            k = BATCH * step + member
            spectrum = spectra[member * HALF : (member + 1) * HALF]
            if with_edge:
                edge_ref[sub, k, 0:1, :] = spectrum[0:1, :]
                edge_ref[sub, k, 1:2, :] = spectrum[SUB : SUB + 1, :]
            q_real, q_imag = spectrum[:SUB, :LANES], spectrum[:SUB, LANES:]
            u_real, u_imag = spectrum[SUB:, :LANES], spectrum[SUB:, LANES:]
            row = lane * OUTER + k
            fy = jnp.where(row >= extent // 2, row - extent, row).astype(jnp.float32)
            radius = jnp.maximum(fx * fx + fy * fy, 1.0)
            cos_twice = (fx * fx - fy * fy) / radius
            sin_twice = 2.0 * fx * fy / radius

            def powers(sine, which):
                e_real = cos_twice * q_real + sine * u_real
                e_imag = cos_twice * q_imag + sine * u_imag
                b_real = cos_twice * u_real - sine * q_real
                b_imag = cos_twice * u_imag - sine * q_imag
                power_ref[member, which, 0] = (e_real * e_real + e_imag * e_imag) * inv_area * keep
                power_ref[member, which, 1] = (b_real * b_real + b_imag * b_imag) * inv_area * keep
                power_ref[member, which, 2] = (e_real * b_real + e_imag * b_imag) * inv_area * keep

            other = 0
            if member == 0:
                other = jnp.where(k == 0, 1, 0)
                powers(sin_twice, jnp.where(k == 0, 1 - flipped, 0))

                @pl.when(k == 0)
                def _():
                    powers(jnp.where(row == extent // 2, -sin_twice, sin_twice), flipped)

            else:
                powers(sin_twice, 0)

            for index, (bins_ref, begin, count) in enumerate(
                ((bins0_ref, begin0, near), (bins1_ref, begin1, near + 1))
            ):
                for source in range(count):
                    at = min(begin + source, bins_ref.shape[0] - 1)
                    value = bins_ref[at, 0, k]
                    high = jnp.floor(value * (1.0 / LOWS))
                    rows = slice(source * width, (source + 1) * width)
                    part_ref[member, index, 0, rows] = high
                    part_ref[member, index, 1, rows] = value - high * LOWS

            for i in range(SUB):
                mirror = offset - HALF + SUB - i
                for index, at, source in ((0, i, 0), (1, mirror, other)):
                    high = part_ref[member, index, 0, pl.ds(at, 1), :]
                    low = part_ref[member, index, 1, pl.ds(at, 1), :]
                    high = jnp.broadcast_to(high, (GROUPS, LANES)).astype(jnp.bfloat16)
                    low = jnp.broadcast_to(low, (LOWS, LANES)).astype(jnp.bfloat16)
                    hot = high == group_iota
                    column = []
                    for kind in range(3):
                        power = power_ref[member, source, kind, pl.ds(i, 1), :]
                        power = jnp.broadcast_to(power, (GROUPS, LANES)).astype(jnp.bfloat16)
                        column.append(jnp.where(hot, power, empty))
                    weighted.append(jnp.concatenate(column, 0))
                    lows.append(jnp.where(low == low_iota, one, none))
        return acc + dot_f32(
            jnp.concatenate(weighted, 1), jnp.concatenate(lows, 1), (((1,), (1,)), ((), ()))
        )

    sums_ref[0] = lax.fori_loop(0, OUTER // BATCH, batch, jnp.zeros((3 * GROUPS, LOWS), jnp.float32))


def summed(array, axis):
    distance = 0
    while 1 << distance < lax.axis_size(axis):
        array = array + partner(array, axis, distance)
        distance += 1
    return array


def edge_sums(edge, bins_left, bins_right, extent):
    flat = edge.transpose(1, 2, 0).reshape(2, 2, extent)
    back = jnp.roll(flat[:, :, ::-1], 1, axis=2)
    q_real, q_imag, u_real, u_imag = [
        jnp.stack(pair)
        for m in range(2)
        for pair in (
            (0.5 * (flat[m, 0] + back[m, 0]), 0.5 * (flat[m, 1] + back[m, 1])),
            (0.5 * (flat[m, 1] - back[m, 1]), 0.5 * (back[m, 0] - flat[m, 0])),
        )
    ]
    freq_y = signed_float(lax.iota(jnp.int32, extent), extent)[None, :]
    freq_x = jnp.array([0.0, -extent // 2], jnp.float32)[:, None]
    left = bins_left.T.reshape(extent)
    right = jnp.roll(bins_right.T.reshape(extent)[::-1], 1)
    bins = jnp.stack([left, right]).astype(jnp.int32)
    return band_terms((q_real, q_imag, u_real, u_imag), freq_y, freq_x, bins, NBINS, extent)


def on_device_fast(maps, mask, bins):
    extent = bins.shape[0]
    columns = bins.shape[1]
    count = maps.shape[1]
    slabs = lax.axis_size("rows")
    reps = lax.axis_size("rep")
    slab_index = lax.axis_index("rows")
    member = lax.axis_index("rep")
    pair_bit = member % 2
    half_slabs = slabs // 2
    first, family, natural = host_tables(extent)
    row_high, row_low = split_table(np.stack([first, family]))
    col_high, col_low = split_table(natural)

    flips = np.zeros((2, 2 * LANES, LANES))
    for k in range(LANES):
        flips[0, k, -k % LANES] = 8.0
        flips[0, LANES + k, -k % LANES] = 1.0
        flips[1, k, LANES - 1 - k] = 8.0
        flips[1, LANES + k, LANES - 1 - k] = 1.0
    info = jnp.stack([pair_bit, (slab_index >= half_slabs).astype(jnp.int32)])
    sub = 8
    width = columns // OUTER
    sent_bins = pl.pallas_call(
        bins_kernel,
        grid=(OUTER // sub,),
        in_specs=[
            pl.BlockSpec(memory_space=pltpu.SMEM),
            pl.BlockSpec((2, 2 * LANES, LANES), lambda i: (0, 0, 0)),
        ]
        + [
            pl.BlockSpec((LANES, sub, LANES), lambda i, part=part: (0, i, part))
            for part in range(columns // LANES)
        ],
        out_specs=pl.BlockSpec((slabs, 2, OUTER, width, LANES), lambda i: (0, 0, 0, 0, 0)),
        out_shape=jax.ShapeDtypeStruct((slabs, 2, OUTER, width, LANES), jnp.float32),
        scratch_shapes=[pltpu.VMEM((2, columns, LANES), jnp.float32)],
        cost_estimate=pl.CostEstimate(flops=5 * 10**9, transcendentals=0, bytes_accessed=12 * 2**20),
        name="bins_prep",
    )(info, jnp.asarray(flips, jnp.bfloat16), *[bins.reshape(LANES, OUTER, columns)] * (columns // LANES))
    got_bins = lax.all_to_all(sent_bins, "rows", split_axis=0, concat_axis=0, tiled=True)

    block = min(LANES, count)
    k1 = np.arange(OUTER // 2)[:, None]
    angles = 2 * np.pi * (k1 * np.arange(LANES)[None, :] % extent) / extent
    turns = jnp.asarray(np.stack([np.cos(angles), -np.sin(angles)]), jnp.float32)
    table_spec = pl.BlockSpec((2, 2 * LANES, 2 * LANES), lambda i: (0, 0, 0))
    piece = jax.ShapeDtypeStruct((2 * slabs, count // 2, LANES), jnp.float32)
    piece_spec = pl.BlockSpec((2 * slabs, block // 2, LANES), lambda i: (0, i, 0))
    pieces = pl.pallas_call(
        row_kernel,
        grid=(count // block,),
        in_specs=[
            pl.BlockSpec((1, block, extent), lambda i: (0, i, 0)),
            pl.BlockSpec((block, extent), lambda i: (i, 0)),
            pl.BlockSpec(turns.shape, lambda i: (0, 0, 0)),
            table_spec,
            table_spec,
        ],
        out_specs=[piece_spec] * (LANES // SUB),
        out_shape=[piece] * (LANES // SUB),
        scratch_shapes=[pltpu.VMEM((OUTER // 2, block, 2 * LANES), jnp.float32)],
        cost_estimate=pl.CostEstimate(flops=12 * 10**9, transcendentals=0, bytes_accessed=24 * 2**20),
        name="row_fft",
    )(maps, mask, turns, row_high, row_low)

    groups = [
        [row * reps + z for row in range(slabs) for z in (2 * sky, 2 * sky + 1)]
        for sky in range(reps // 2)
    ]
    fam = 2 * slab_index + pair_bit
    angles = np.arange(HALF)[:, None] + HALF * (np.arange(LANES)[None, :] >= HALF)
    angles = 2 * np.pi * angles / extent
    spin = jnp.asarray(np.stack([np.cos(angles), -np.sin(angles)]), jnp.float32)
    slots = lax.iota(jnp.int32, HALF)
    zero = (fam == 0).astype(jnp.int32)
    total = None
    for number, piece in enumerate(pieces):
        chunk, half_chunk = number // 2, number % 2
        got = lax.all_to_all(
            piece, ("rows", "rep"), split_axis=0, concat_axis=0, tiled=True,
            axis_index_groups=groups,
        )
        got = got.reshape(slabs, 2, -1, count // 2, LANES)
        subs = got.shape[2]
        first_col = OUTER * slots if chunk == 0 else OUTER // 2 + OUTER * (HALF - 1 - slots)
        col = jnp.where(fam == 0, first_col, fam + OUTER * (slots + HALF * chunk))
        col = col[half_chunk * SUB : (half_chunk + 1) * SUB]
        fx = jnp.broadcast_to(signed_float(col, extent).reshape(subs, SUB, 1), (subs, SUB, LANES))
        with_edge = number == 0
        if chunk == 0:
            info = jnp.stack([HALF - 1 + zero, jnp.int32(1), zero])
        else:
            info = jnp.stack([jnp.int32(HALF - 1), 1 - zero, jnp.int32(0)])
        if number == 1:
            info, special = lax.optimization_barrier((info, special))
        bin_block = (half_slabs, 1, OUTER, width, LANES)
        edge_shape = (subs, OUTER, 2, 2 * LANES)
        sums_shape = (subs, 3 * GROUPS, LOWS)
        band_call = pl.pallas_call(
            functools.partial(band_kernel, extent, half_chunk, with_edge),
            grid=(subs,),
            in_specs=[
                pl.BlockSpec(memory_space=pltpu.SMEM),
                pl.BlockSpec((slabs, 2, 1, count // 2, LANES), lambda i: (0, 0, i, 0, 0)),
                pl.BlockSpec(bin_block, lambda i, at=chunk: (at, 0, 0, 0, 0)),
                pl.BlockSpec(bin_block, lambda i, at=1 - chunk: (at, 1, 0, 0, 0)),
                pl.BlockSpec(spin.shape, lambda i: (0, 0, 0)),
                pl.BlockSpec(col_high.shape, lambda i: (0, 0)),
                pl.BlockSpec(col_low.shape, lambda i: (0, 0)),
                pl.BlockSpec((1, SUB, LANES), lambda i: (i, 0, 0)),
            ],
            out_specs=[pl.BlockSpec((1, 3 * GROUPS, LOWS), lambda i: (i, 0, 0))]
            + [pl.BlockSpec(edge_shape, lambda i: (0, 0, 0, 0))] * with_edge,
            out_shape=[jax.ShapeDtypeStruct(sums_shape, jnp.float32)]
            + [jax.ShapeDtypeStruct(edge_shape, jnp.float32)] * with_edge,
            scratch_shapes=[
                pltpu.VMEM((OUTER, LANES, LANES), jnp.float32),
                pltpu.VMEM((BATCH, 2, 3, SUB, LANES), jnp.float32),
                pltpu.VMEM((BATCH, 2, 2, SUB + width, LANES), jnp.float32),
            ],
            compiler_params=pltpu.CompilerParams(vmem_limit_bytes=48 * 2**20),
            cost_estimate=pl.CostEstimate(flops=10**10, transcendentals=0, bytes_accessed=4 * 2**20),
            name="band_sums",
        )
        out = band_call(info, got, got_bins, got_bins, spin, col_high, col_low, fx)
        sums = out[0].sum(0)
        total = sums if total is None else total + sums
        if with_edge:
            special = edge_sums(
                out[1][0], got_bins[0, 0, :, 0], got_bins[half_slabs, 1, :, 0], extent
            )
            special = jnp.where(fam == 0, special, 0.0)
    partial_sums = total.reshape(3, NBINS) + special
    auto = NBINS / (extent * extent)
    cross = math.sqrt(auto)
    factors = jnp.array([auto, auto, cross], jnp.float32)[:, None]
    own = summed(partial_sums, "rows")

    own = (own + partner(own, "rep", 0)) * factors
    skies = [own]
    distance = 1
    while 1 << distance < reps:
        skies = skies + [partner(sky, "rep", distance) for sky in skies]
        distance += 1
    stacked = jnp.stack(skies)
    order = lax.iota(jnp.int32, len(skies)) ^ (member // 2)
    return jnp.take(stacked, order, axis=0) if len(skies) > 2 else jnp.where(
        member // 2 == 0, stacked, stacked[::-1]
    )


def solution(mesh):
    in_specs = (P("rep", "rows", None), P("rows", None), P(None, "rows"))
    out_specs = P()

    def on_any(maps, mask, bins):
        extent = bins.shape[0]
        families = 2 * lax.axis_size("rows")
        if extent == OUTER * LANES and families == OUTER // 2 and NBINS == GROUPS * LOWS:
            return on_device_fast(maps, mask, bins)
        return on_device(maps, mask, bins)

    return jax.shard_map(
        on_any, mesh=mesh, in_specs=in_specs, out_specs=out_specs, check_vma=False
    )
```
